128 devices in a mesh: rows: 16 (over z, y), cols: 8 (over x, core).
Axes of the slice: x: 4, y: 4, z: 4, core: 2. Of those that a mesh axis runs over, the one named last changes fastest.
Arguments:
- grad_stack: float32 [512, 64, 2048], P(None, 'rows', 'cols'), may hold values from -6 to 6
- moment_stack: float32 [512, 64, 2048], P(None, 'rows', 'cols'), may hold values from -6 to 6
- weight_stack: float32 [512, 64, 2048], P(None, 'rows', 'cols'), may hold values from -0.1875 to 0.1875
Outputs:
- new_weights: float32 [512, 64, 2048], P(None, 'rows', 'cols')
- new_momentum: float32 [512, 64, 2048], P(None, 'rows', 'cols')
The draws below stay inside these ranges and needn't reach their ends.
All inputs are finite; a program needn't handle non-finite values.
Results may differ from the reference program's by a relative error of at most 0.0003.
Values sent between devices are 32-bit elements.
A program may use at most 128 MiB of HBM per device.

```python
import jax
import jax.numpy as jnp
from jax import lax

SIDE = 64
WIDE = 2048
MATS = 512
ITERS = 5


def block_levels(rng, extent, shards, least, high):
    loudness, own = 1.0, jax.random.fold_in(rng, 6)
    for axis_at, shards_of in shards:
        steps = jnp.exp(jax.random.uniform(jax.random.fold_in(own, axis_at), (shards_of,), jnp.float32, least / len(shards), high / len(shards)))
        loudness = loudness * jnp.repeat(steps, extent[axis_at] // shards_of).reshape([-1 if axis == axis_at else 1 for axis in range(len(extent))])
    return loudness


def centred(own_key, dims, spread, most, cuts=(), dtype=jnp.bfloat16):
    loudness = block_levels(own_key, dims, cuts, -0.22, 0.18) if cuts else 1.0
    array = jax.random.normal(own_key, dims, jnp.float32) * spread * loudness
    return jnp.minimum(jnp.maximum(array, -most), most).astype(dtype)


def setup_inputs(seed: int = 0) -> dict:
    key_list = jax.random.split(jax.random.key(seed), 4)
    return {
        "grad_stack": centred(key_list[0], (MATS, SIDE, WIDE), 1.0, 6.0, ((1, 16), (2, 8)), jnp.float32),
        "moment_stack": centred(key_list[1], (MATS, SIDE, WIDE), 1.0, 6.0, ((1, 16), (2, 8)), jnp.float32),
        "weight_stack": centred(key_list[2], (MATS, SIDE, WIDE), 0.03, 0.1875, ((1, 16), (2, 8)), jnp.float32),
    }


hold_rate = 0.95
learn_rate = 1.0

def reference(grad_stack, moment_stack, weight_stack):
    new_momentum = hold_rate * moment_stack + grad_stack

    def orthogonal_one(stack):
        iterate = stack[None]
        iterate = iterate * lax.rsqrt(lax.optimization_barrier(jnp.sum(iterate * iterate, axis=(1, 2), keepdims=True)) + 1e-06)
        for step in range(ITERS):
            gram = jnp.einsum('mik,mjk->mij', iterate, iterate, precision=lax.Precision.HIGHEST)
            mixed = -4.775 * gram + 2.0315 * jnp.einsum('mij,mjk->mik', gram, gram, precision=lax.Precision.HIGHEST)
            iterate = 3.4445 * iterate + jnp.einsum('mij,mjk->mik', mixed, iterate, precision=lax.Precision.HIGHEST)
        return iterate[0]
    iterate = lax.map(orthogonal_one, new_momentum)
    new_weights = weight_stack - learn_rate * iterate
    return (new_weights, new_momentum)
```

```python
import functools
import itertools

import jax
import jax.numpy as jnp
from jax import lax
from jax.experimental import pallas as pl
from jax.experimental.pallas import tpu as pltpu
from jax.sharding import PartitionSpec as P

hold_rate = 0.95
learn_rate = 1.0
LINEAR, CUBIC, QUINTIC = 3.4445, -4.775, 2.0315

MESH = pl.DeviceIdType.MESH
STAGES = 2
HIGHEST = lax.Precision.HIGHEST


def send_order():
    def put(axes, values):
        offset = [0, 0, 0]
        for axis, value in zip(axes, values):
            offset[axis] = value % 4
        return tuple(offset)

    rounds = [[(2, 2, 2)]]
    for a, b in itertools.product((1, -1), repeat=2):
        rounds.append([put((0, 1, 2), (1, a, b)), put((0, 1, 2), (-1, -a, -b))])
    for d in range(3):
        e, f = [axis for axis in range(3) if axis != d]
        for a, b in itertools.product((1, -1), repeat=2):
            rounds.append([put((d, e, f), (2, a, b)), put((d, e, f), (0, -a, -b))])
        for a in (1, -1):
            rounds.append([put((d, e, f), (a, 2, 2)), put((d, e, f), (-a, 0, 0))])
        rounds.append([put((d, e, f), (0, 2, 2)), put((d, e, f), (2, 0, 0))])
        for a in (1, -1):
            rounds.append([put((d, e, f), (a, 2, 0)), put((d, e, f), (-a, 0, 2))])
    order = [(0, 0, 0, 1)]
    for group in rounds:
        for core in range(2):
            order += [offset + (core,) for offset in group]
    assert len(set(order)) == 127
    return order


ORDER = send_order()


def mixing(gram, eye, steps):
    mix = None
    for step in range(steps):
        square = jnp.dot(gram, gram, precision=HIGHEST)
        poly = LINEAR * eye + CUBIC * gram + QUINTIC * square
        mix = poly if mix is None else jnp.dot(poly, mix, precision=HIGHEST)
        if step < steps - 1:
            gram = jnp.dot(poly, jnp.dot(gram, poly, precision=HIGHEST), precision=HIGHEST)
    return mix


def kernel(x_ref, out_ref, taken, made, sent, got, back_sent, back_got):
    row, col = lax.axis_index("rows"), lax.axis_index("cols")
    z, y, x, core = row // 4, row % 4, col // 2, col % 2
    zs = [lax.rem(z + d, 4) for d in range(4)]
    ys = [lax.rem(y + d, 4) for d in range(4)]
    xs = [lax.rem(x + d, 4) for d in range(4)]
    cores = [core, 1 - core]
    rows = {(a, b): zs[a] * 4 + ys[b] for a in range(4) for b in range(4)}
    cols = {(a, b): xs[a] * 2 + cores[b] for a in range(4) for b in range(2)}
    places = [(rows[dz, dy], cols[dx, dc]) for dz, dy, dx, dc in ORDER]
    each = 4 // STAGES
    me = row * 8 + col

    barrier = pltpu.get_barrier_semaphore()
    for place in places:
        pl.semaphore_signal(barrier, inc=1, device_id=place, device_id_type=MESH)
    pl.semaphore_wait(barrier, len(places))

    for stage in range(STAGES):
        pltpu.make_async_copy(
            x_ref.at[pl.ds(me * 4 + stage * each, each)], taken.at[stage, row, col], got.at[stage]
        ).start()
        for place in places:
            pltpu.make_async_remote_copy(
                src_ref=x_ref.at[pl.ds((place[0] * 8 + place[1]) * 4 + stage * each, each)],
                dst_ref=taken.at[stage, row, col],
                send_sem=sent.at[stage],
                recv_sem=got.at[stage],
                device_id=place,
                device_id_type=MESH,
            ).start()

    up = lax.broadcasted_iota(jnp.int32, (128, 128), 0)
    across = lax.broadcasted_iota(jnp.int32, (128, 128), 1)
    same_half = (up // 4) % 2 == (across // 4) % 2
    upper = (across // 4) % 2 == 1
    eye = jnp.where(up == across, 1.0, 0.0).astype(jnp.float32)

    def gram_of(blocks):
        wide = jnp.concatenate(blocks, axis=1)
        both = lax.dot_general(wide, wide, (((1,), (1,)), ((), ())), precision=HIGHEST)
        both = jnp.where(same_half, both, 0.0)
        other = pltpu.roll(both.reshape(16, 8, 128), 4, 1).reshape(128, 128)
        other = jnp.where(upper, pltpu.roll(other, 4, 1), pltpu.roll(other, 124, 1))
        return both + other

    for stage in range(STAGES):
        pltpu.make_async_copy(taken.at[stage], taken.at[stage], got.at[stage]).wait()
        for mat in range(each):
            blocks = [taken[stage, :, c, mat].reshape(128, 128) for c in range(8)]
            gram = gram_of(blocks)
            total = 0.5 * jnp.sum(jnp.where(up == across, gram, 0.0), keepdims=True)
            scale = lax.rsqrt(total + 1e-06)
            mix = mixing(gram * (scale * scale), eye, 2) * scale
            blocks = [jnp.dot(mix, block, precision=HIGHEST) for block in blocks]
            mix = mixing(gram_of(blocks), eye, 3)
            for c in range(8):
                made[stage, :, c, mat] = jnp.dot(mix, blocks[c], precision=HIGHEST).reshape(16, 8, 128)
        pltpu.make_async_copy(
            made.at[stage, row, col], out_ref.at[pl.ds(me * 4 + stage * each, each)], back_got.at[stage]
        ).start()
        for place in places:
            pltpu.make_async_remote_copy(
                src_ref=made.at[stage, place[0], place[1]],
                dst_ref=out_ref.at[pl.ds(me * 4 + stage * each, each)],
                send_sem=back_sent.at[stage],
                recv_sem=back_got.at[stage],
                device_id=place,
                device_id_type=MESH,
            ).start()

    whole = out_ref.at[pl.ds(0, 128 * each)]
    part = out_ref.at[pl.ds(0, 127 * each)]
    for stage in range(STAGES):
        pltpu.make_async_copy(whole, whole, back_got.at[stage]).wait()
    for stage in range(STAGES):
        pltpu.make_async_copy(part, part, sent.at[stage]).wait()
        pltpu.make_async_copy(part, part, back_sent.at[stage]).wait()


def on_device(grad_stack, moment_stack, weight_stack):
    mats = grad_stack.shape[0]
    new_momentum = hold_rate * moment_stack + grad_stack
    tiles = new_momentum.reshape(mats, 4, 2, 128).transpose(0, 2, 1, 3).reshape(mats, 8, 128)
    each = 4 // STAGES
    back = pl.pallas_call(
        kernel,
        out_shape=jax.ShapeDtypeStruct((mats, 8, 128), jnp.float32),
        in_specs=[pl.BlockSpec(memory_space=pltpu.VMEM)],
        out_specs=pl.BlockSpec(memory_space=pltpu.VMEM),
        scratch_shapes=[
            pltpu.VMEM((STAGES, 16, 8, each, 8, 128), jnp.float32),
            pltpu.VMEM((STAGES, 16, 8, each, 8, 128), jnp.float32),
            pltpu.SemaphoreType.DMA((STAGES,)),
            pltpu.SemaphoreType.DMA((STAGES,)),
            pltpu.SemaphoreType.DMA((STAGES,)),
            pltpu.SemaphoreType.DMA((STAGES,)),
        ],
        compiler_params=pltpu.CompilerParams(
            collective_id=1, has_side_effects=True, vmem_limit_bytes=48 * 1024 * 1024
        ),
    )(tiles)
    back = back.reshape(mats, 2, 4, 128).transpose(0, 2, 1, 3).reshape(mats, 4, 256)
    new_weights = weight_stack - learn_rate * back
    return (new_weights, new_momentum)


def solution(mesh):
    placed = (P(None, "rows", "cols"), P(None, "rows", "cols"), P(None, "rows", "cols"))
    return jax.shard_map(
        on_device,
        mesh=mesh,
        in_specs=placed,
        out_specs=(P(None, "rows", "cols"), P(None, "rows", "cols")),
        check_vma=False,
    )
```

```python
import functools
import itertools

import jax
import jax.numpy as jnp
from jax import lax
from jax.experimental import pallas as pl
from jax.experimental.pallas import tpu as pltpu
from jax.sharding import PartitionSpec as P

hold_rate = 0.95
learn_rate = 1.0
LINEAR, CUBIC, QUINTIC = 3.4445, -4.775, 2.0315

MESH = pl.DeviceIdType.MESH
STAGES = 4
HIGHEST = lax.Precision.HIGHEST


def send_order():
    def put(axes, values):
        offset = [0, 0, 0]
        for axis, value in zip(axes, values):
            offset[axis] = value % 4
        return tuple(offset)

    rounds = [[(2, 2, 2)]]
    for a, b in itertools.product((1, -1), repeat=2):
        rounds.append([put((0, 1, 2), (1, a, b)), put((0, 1, 2), (-1, -a, -b))])
    for d in range(3):
        e, f = [axis for axis in range(3) if axis != d]
        for a, b in itertools.product((1, -1), repeat=2):
            rounds.append([put((d, e, f), (2, a, b)), put((d, e, f), (0, -a, -b))])
        for a in (1, -1):
            rounds.append([put((d, e, f), (a, 2, 2)), put((d, e, f), (-a, 0, 0))])
        rounds.append([put((d, e, f), (0, 2, 2)), put((d, e, f), (2, 0, 0))])
        for a in (1, -1):
            rounds.append([put((d, e, f), (a, 2, 0)), put((d, e, f), (-a, 0, 2))])
    order = [(0, 0, 0, 1)]
    for group in rounds:
        for core in range(2):
            order += [offset + (core,) for offset in group]
    assert len(set(order)) == 127
    return order


ORDER = send_order()


def mixing(gram, eye, steps):
    mix = None
    for step in range(steps):
        square = jnp.dot(gram, gram, precision=HIGHEST)
        poly = LINEAR * eye + CUBIC * gram + QUINTIC * square
        mix = poly if mix is None else jnp.dot(poly, mix, precision=HIGHEST)
        if step < steps - 1:
            gram = jnp.dot(poly, jnp.dot(gram, poly, precision=HIGHEST), precision=HIGHEST)
    return mix


def kernel(x_ref, out_ref, taken, made, sent, got, back_sent, back_got):
    row, col = lax.axis_index("rows"), lax.axis_index("cols")
    z, y, x, core = row // 4, row % 4, col // 2, col % 2
    zs = [lax.rem(z + d, 4) for d in range(4)]
    ys = [lax.rem(y + d, 4) for d in range(4)]
    xs = [lax.rem(x + d, 4) for d in range(4)]
    cores = [core, 1 - core]
    rows = {(a, b): zs[a] * 4 + ys[b] for a in range(4) for b in range(4)}
    cols = {(a, b): xs[a] * 2 + cores[b] for a in range(4) for b in range(2)}
    places = [(rows[dz, dy], cols[dx, dc]) for dz, dy, dx, dc in ORDER]
    each = 4 // STAGES
    me = row * 8 + col

    barrier = pltpu.get_barrier_semaphore()
    for place in places:
        pl.semaphore_signal(barrier, inc=1, device_id=place, device_id_type=MESH)
    pl.semaphore_wait(barrier, len(places))

    for stage in range(STAGES):
        pltpu.make_async_copy(
            x_ref.at[pl.ds(me * 4 + stage * each, each)], taken.at[stage, row, col], got.at[stage]
        ).start()
        for place in places:
            pltpu.make_async_remote_copy(
                src_ref=x_ref.at[pl.ds((place[0] * 8 + place[1]) * 4 + stage * each, each)],
                dst_ref=taken.at[stage, row, col],
                send_sem=sent.at[stage],
                recv_sem=got.at[stage],
                device_id=place,
                device_id_type=MESH,
            ).start()

    up = lax.broadcasted_iota(jnp.int32, (128, 128), 0)
    across = lax.broadcasted_iota(jnp.int32, (128, 128), 1)
    same_half = (up // 4) % 2 == (across // 4) % 2
    upper = (across // 4) % 2 == 1
    eye = jnp.where(up == across, 1.0, 0.0).astype(jnp.float32)

    def gram_of(blocks):
        wide = jnp.concatenate(blocks, axis=1)
        both = lax.dot_general(wide, wide, (((1,), (1,)), ((), ())), precision=HIGHEST)
        both = jnp.where(same_half, both, 0.0)
        other = pltpu.roll(both.reshape(16, 8, 128), 4, 1).reshape(128, 128)
        other = jnp.where(upper, pltpu.roll(other, 4, 1), pltpu.roll(other, 124, 1))
        return both + other

    for stage in range(STAGES):
        pltpu.make_async_copy(taken.at[stage], taken.at[stage], got.at[stage]).wait()
        for mat in range(each):
            blocks = [taken[stage, :, c, mat].reshape(128, 128) for c in range(8)]
            gram = gram_of(blocks)
            total = 0.5 * jnp.sum(jnp.where(up == across, gram, 0.0), keepdims=True)
            scale = lax.rsqrt(total + 1e-06)
            mix = mixing(gram * (scale * scale), eye, 2) * scale
            blocks = [jnp.dot(mix, block, precision=HIGHEST) for block in blocks]
            mix = mixing(gram_of(blocks), eye, 3)
            for c in range(8):
                made[stage, :, c, mat] = jnp.dot(mix, blocks[c], precision=HIGHEST).reshape(16, 8, 128)
        pltpu.make_async_copy(
            made.at[stage, row, col], out_ref.at[pl.ds(me * 4 + stage * each, each)], back_got.at[stage]
        ).start()
        for place in places:
            pltpu.make_async_remote_copy(
                src_ref=made.at[stage, place[0], place[1]],
                dst_ref=out_ref.at[pl.ds(me * 4 + stage * each, each)],
                send_sem=back_sent.at[stage],
                recv_sem=back_got.at[stage],
                device_id=place,
                device_id_type=MESH,
            ).start()

    whole = out_ref.at[pl.ds(0, 128 * each)]
    part = out_ref.at[pl.ds(0, 127 * each)]
    for stage in range(STAGES):
        pltpu.make_async_copy(whole, whole, back_got.at[stage]).wait()
    for stage in range(STAGES):
        pltpu.make_async_copy(part, part, sent.at[stage]).wait()
        pltpu.make_async_copy(part, part, back_sent.at[stage]).wait()


def on_device(grad_stack, moment_stack, weight_stack):
    mats = grad_stack.shape[0]
    new_momentum = hold_rate * moment_stack + grad_stack
    tiles = new_momentum.reshape(mats, 4, 2, 128).transpose(0, 2, 1, 3).reshape(mats, 8, 128)
    each = 4 // STAGES
    back = pl.pallas_call(
        kernel,
        out_shape=jax.ShapeDtypeStruct((mats, 8, 128), jnp.float32),
        in_specs=[pl.BlockSpec(memory_space=pltpu.VMEM)],
        out_specs=pl.BlockSpec(memory_space=pltpu.VMEM),
        scratch_shapes=[
            pltpu.VMEM((STAGES, 16, 8, each, 8, 128), jnp.float32),
            pltpu.VMEM((STAGES, 16, 8, each, 8, 128), jnp.float32),
            pltpu.SemaphoreType.DMA((STAGES,)),
            pltpu.SemaphoreType.DMA((STAGES,)),
            pltpu.SemaphoreType.DMA((STAGES,)),
            pltpu.SemaphoreType.DMA((STAGES,)),
        ],
        compiler_params=pltpu.CompilerParams(
            collective_id=1, has_side_effects=True, vmem_limit_bytes=48 * 1024 * 1024
        ),
    )(tiles)
    back = back.reshape(mats, 2, 4, 128).transpose(0, 2, 1, 3).reshape(mats, 4, 256)
    new_weights = weight_stack - learn_rate * back
    return (new_weights, new_momentum)


def solution(mesh):
    placed = (P(None, "rows", "cols"), P(None, "rows", "cols"), P(None, "rows", "cols"))
    return jax.shard_map(
        on_device,
        mesh=mesh,
        in_specs=placed,
        out_specs=(P(None, "rows", "cols"), P(None, "rows", "cols")),
        check_vma=False,
    )
```

```python
import itertools

import jax
import jax.numpy as jnp
from jax import lax
from jax.experimental import pallas as pl
from jax.experimental.pallas import tpu as pltpu
from jax.sharding import PartitionSpec as P

hold_rate = 0.95
learn_rate = 1.0
LINEAR, CUBIC, QUINTIC = 3.4445, -4.775, 2.0315

MESH = pl.DeviceIdType.MESH
STAGES = 4
PIECE = 16
HIGHEST = lax.Precision.HIGHEST


def send_order():
    def put(axes, values):
        offset = [0, 0, 0]
        for axis, value in zip(axes, values):
            offset[axis] = value % 4
        return tuple(offset)

    rounds = [[(2, 2, 2)]]
    for a, b in itertools.product((1, -1), repeat=2):
        rounds.append([put((0, 1, 2), (1, a, b)), put((0, 1, 2), (-1, -a, -b))])
    for d in range(3):
        e, f = [axis for axis in range(3) if axis != d]
        for a, b in itertools.product((1, -1), repeat=2):
            rounds.append([put((d, e, f), (2, a, b)), put((d, e, f), (0, -a, -b))])
        for a in (1, -1):
            rounds.append([put((d, e, f), (a, 2, 2)), put((d, e, f), (-a, 0, 0))])
        rounds.append([put((d, e, f), (0, 2, 2)), put((d, e, f), (2, 0, 0))])
        for a in (1, -1):
            rounds.append([put((d, e, f), (a, 2, 0)), put((d, e, f), (-a, 0, 2))])
    order = [(0, 0, 0, 1)]
    for group in rounds:
        for core in range(2):
            order += [offset + (core,) for offset in group]
    assert len(set(order)) == 127
    return order


ORDER = send_order()


def mixing(gram, eye, steps):
    mix = None
    for step in range(steps):
        square = jnp.dot(gram, gram, precision=HIGHEST)
        poly = LINEAR * eye + CUBIC * gram + QUINTIC * square
        mix = poly if mix is None else jnp.dot(poly, mix, precision=HIGHEST)
        if step < steps - 1:
            gram = jnp.dot(poly, jnp.dot(gram, poly, precision=HIGHEST), precision=HIGHEST)
    return mix


def kernel(
    grad_ref, moment_ref, weight_ref, out_ref, x_ref,
    grad, moment, taken, made, landed, sent, got, back_sent, back_got, loaded, held,
):
    row, col = lax.axis_index("rows"), lax.axis_index("cols")
    z, y, x, core = row // 4, row % 4, col // 2, col % 2
    zs = [lax.rem(z + d, 4) for d in range(4)]
    ys = [lax.rem(y + d, 4) for d in range(4)]
    xs = [lax.rem(x + d, 4) for d in range(4)]
    cores = [core, 1 - core]
    rows = {(a, b): zs[a] * 4 + ys[b] for a in range(4) for b in range(4)}
    cols = {(a, b): xs[a] * 2 + cores[b] for a in range(4) for b in range(2)}
    places = [(rows[dz, dy], cols[dx, dc]) for dz, dy, dx, dc in ORDER]
    me = row * 8 + col

    pieces = [pl.ds(piece * PIECE, PIECE) for piece in range(128 // PIECE)]
    loads = []
    for at, piece in enumerate(pieces):
        loads.append((
            pltpu.make_async_copy(grad_ref.at[piece], grad.at[piece], loaded.at[0, at]),
            pltpu.make_async_copy(moment_ref.at[piece], moment.at[piece], loaded.at[1, at]),
        ))
    for pair in loads:
        for load in pair:
            load.start()
    weights = pltpu.make_async_copy(weight_ref, out_ref, held)
    weights.start()

    barrier = pltpu.get_barrier_semaphore()
    for place in places:
        pl.semaphore_signal(barrier, inc=1, device_id=place, device_id_type=MESH)
    for piece, pair in zip(pieces, loads):
        for load in pair:
            load.wait()
        x_ref[piece] = hold_rate * moment[piece] + grad[piece]
    pl.semaphore_wait(barrier, len(places))

    for stage in range(STAGES):
        pltpu.make_async_copy(x_ref.at[me, stage], taken.at[stage, row, col], got.at[stage]).start()
        for place in places:
            pltpu.make_async_remote_copy(
                src_ref=x_ref.at[place[0] * 8 + place[1], stage],
                dst_ref=taken.at[stage, row, col],
                send_sem=sent.at[stage],
                recv_sem=got.at[stage],
                device_id=place,
                device_id_type=MESH,
            ).start()

    up = lax.broadcasted_iota(jnp.int32, (128, 128), 0)
    across = lax.broadcasted_iota(jnp.int32, (128, 128), 1)
    same_half = (up // 4) % 2 == (across // 4) % 2
    upper = (across // 4) % 2 == 1
    eye = jnp.where(up == across, 1.0, 0.0).astype(jnp.float32)

    def gram_of(blocks):
        wide = jnp.concatenate(blocks, axis=1)
        both = lax.dot_general(wide, wide, (((1,), (1,)), ((), ())), precision=HIGHEST)
        both = jnp.where(same_half, both, 0.0)
        other = pltpu.roll(both.reshape(16, 8, 128), 4, 1).reshape(128, 128)
        other = jnp.where(upper, pltpu.roll(other, 4, 1), pltpu.roll(other, 124, 1))
        return both + other

    for stage in range(STAGES):
        pltpu.make_async_copy(taken.at[stage], taken.at[stage], got.at[stage]).wait()
        blocks = [taken[stage, :, c].reshape(128, 128) for c in range(8)]
        gram = gram_of(blocks)
        total = 0.5 * jnp.sum(jnp.where(up == across, gram, 0.0), keepdims=True)
        scale = lax.rsqrt(total + 1e-06)
        mix = mixing(gram * (scale * scale), eye, 2) * scale
        blocks = [jnp.dot(mix, block, precision=HIGHEST) for block in blocks]
        mix = mixing(gram_of(blocks), eye, 3)
        for c in range(8):
            made[stage, :, c] = jnp.dot(mix, blocks[c], precision=HIGHEST).reshape(16, 8, 128)
        pltpu.make_async_copy(made.at[stage, row, col], landed.at[stage, me], back_got.at[stage]).start()
        for place in places:
            pltpu.make_async_remote_copy(
                src_ref=made.at[stage, place[0], place[1]],
                dst_ref=landed.at[stage, me],
                send_sem=back_sent.at[stage],
                recv_sem=back_got.at[stage],
                device_id=place,
                device_id_type=MESH,
            ).start()

    weights.wait()
    for stage in range(STAGES):
        pltpu.make_async_copy(landed.at[stage], landed.at[stage], back_got.at[stage]).wait()
        out_ref[:, stage] = out_ref[:, stage] - learn_rate * landed[stage]
    part = landed.at[0, pl.ds(0, 127)]
    for stage in range(STAGES):
        pltpu.make_async_copy(part, part, sent.at[stage]).wait()
        pltpu.make_async_copy(part, part, back_sent.at[stage]).wait()


def write_out(weights, momentum, weights_out, momentum_out, done):
    copies = [
        pltpu.make_async_copy(weights, weights_out, done.at[0]),
        pltpu.make_async_copy(momentum, momentum_out, done.at[1]),
    ]
    for copy in copies:
        copy.start()
    for copy in copies:
        copy.wait()


def to_tiles(array):
    return array.reshape(512, 4, 2, 128).transpose(0, 2, 1, 3).reshape(128, 4, 8, 128)


def from_tiles(array):
    return array.reshape(512, 2, 4, 128).transpose(0, 2, 1, 3).reshape(512, 4, 256)


def on_device(grad_stack, moment_stack, weight_stack):
    tiles = jax.ShapeDtypeStruct((128, 4, 8, 128), jnp.float32)
    in_vmem = pl.BlockSpec(memory_space=pltpu.VMEM)
    anywhere = pl.BlockSpec(memory_space=pl.ANY)
    updated = pl.pallas_call(
        kernel,
        out_shape=(tiles, tiles),
        in_specs=[anywhere] * 3,
        out_specs=[in_vmem] * 2,
        scratch_shapes=[
            pltpu.VMEM((128, 4, 8, 128), jnp.float32),
            pltpu.VMEM((128, 4, 8, 128), jnp.float32),
            pltpu.VMEM((STAGES, 16, 8, 8, 128), jnp.float32),
            pltpu.VMEM((STAGES, 16, 8, 8, 128), jnp.float32),
            pltpu.VMEM((STAGES, 128, 8, 128), jnp.float32),
            pltpu.SemaphoreType.DMA((STAGES,)),
            pltpu.SemaphoreType.DMA((STAGES,)),
            pltpu.SemaphoreType.DMA((STAGES,)),
            pltpu.SemaphoreType.DMA((STAGES,)),
            pltpu.SemaphoreType.DMA((2, 128 // PIECE)),
            pltpu.SemaphoreType.DMA,
        ],
        compiler_params=pltpu.CompilerParams(
            collective_id=1, has_side_effects=True, vmem_limit_bytes=48 * 1024 * 1024
        ),
    )(to_tiles(grad_stack), to_tiles(moment_stack), to_tiles(weight_stack))
    written = pl.pallas_call(
        write_out,
        out_shape=(tiles, tiles),
        in_specs=[in_vmem] * 2,
        out_specs=[anywhere] * 2,
        scratch_shapes=[pltpu.SemaphoreType.DMA((2,))],
        compiler_params=pltpu.CompilerParams(vmem_limit_bytes=16 * 1024 * 1024),
    )(*updated)
    return tuple(from_tiles(array) for array in written)


def solution(mesh):
    placed = (P(None, "rows", "cols"), P(None, "rows", "cols"), P(None, "rows", "cols"))
    return jax.shard_map(
        on_device,
        mesh=mesh,
        in_specs=placed,
        out_specs=(P(None, "rows", "cols"), P(None, "rows", "cols")),
        check_vma=False,
    )
```

```python
import itertools

import jax
import jax.numpy as jnp
from jax import lax
from jax.experimental import pallas as pl
from jax.experimental.pallas import tpu as pltpu
from jax.sharding import PartitionSpec as P

hold_rate = 0.95
learn_rate = 1.0
LINEAR, CUBIC, QUINTIC = 3.4445, -4.775, 2.0315

MESH = pl.DeviceIdType.MESH
STAGES = 4
PIECE = 16


def send_order():
    def put(axes, values):
        offset = [0, 0, 0]
        for axis, value in zip(axes, values):
            offset[axis] = value % 4
        return tuple(offset)

    rounds = [[(2, 2, 2)]]
    for a, b in itertools.product((1, -1), repeat=2):
        rounds.append([put((0, 1, 2), (1, a, b)), put((0, 1, 2), (-1, -a, -b))])
    for d in range(3):
        e, f = [axis for axis in range(3) if axis != d]
        for a, b in itertools.product((1, -1), repeat=2):
            rounds.append([put((d, e, f), (2, a, b)), put((d, e, f), (0, -a, -b))])
        for a in (1, -1):
            rounds.append([put((d, e, f), (a, 2, 2)), put((d, e, f), (-a, 0, 0))])
        rounds.append([put((d, e, f), (0, 2, 2)), put((d, e, f), (2, 0, 0))])
        for a in (1, -1):
            rounds.append([put((d, e, f), (a, 2, 0)), put((d, e, f), (-a, 0, 2))])
    order = [(0, 0, 0, 1)]
    for group in rounds:
        for core in range(2):
            order += [offset + (core,) for offset in group]
    assert len(set(order)) == 127
    return order


ORDER = send_order()


def parts(array):
    high = array.astype(jnp.bfloat16)
    rest = array - high.astype(jnp.float32)
    middle = rest.astype(jnp.bfloat16)
    return high, middle, (rest - middle.astype(jnp.float32)).astype(jnp.bfloat16)


def product(left, right):
    high, middle, low = left
    high_right, middle_right, low_right = right
    side = lambda *arrays: jnp.concatenate(arrays, axis=1)
    above = lambda *arrays: jnp.concatenate(arrays, axis=0)
    dot = lambda x, y: jnp.dot(x, y, preferred_element_type=jnp.float32)
    large = dot(above(side(high, high), side(middle, middle)), above(high_right, middle_right))
    small = dot(side(low, high), above(high_right, low_right))
    return large[:128] + (large[128:] + small)


def mixing(gram, eye, steps):
    mix = None
    for step in range(steps):
        split = parts(gram)
        poly = LINEAR * eye + CUBIC * gram + QUINTIC * product(split, split)
        split_poly = parts(poly)
        mix = poly if mix is None else product(split_poly, parts(mix))
        if step < steps - 1:
            gram = product(split_poly, parts(product(split_poly, split)))
    return mix


def kernel(
    grad_ref, moment_ref, weight_ref, out_ref, x_ref,
    grad, moment, taken, made, landed, sent, got, back_sent, back_got, loaded, held,
):
    row, col = lax.axis_index("rows"), lax.axis_index("cols")
    z, y, x, core = row // 4, row % 4, col // 2, col % 2
    zs = [lax.rem(z + d, 4) for d in range(4)]
    ys = [lax.rem(y + d, 4) for d in range(4)]
    xs = [lax.rem(x + d, 4) for d in range(4)]
    cores = [core, 1 - core]
    rows = {(a, b): zs[a] * 4 + ys[b] for a in range(4) for b in range(4)}
    cols = {(a, b): xs[a] * 2 + cores[b] for a in range(4) for b in range(2)}
    places = [(rows[dz, dy], cols[dx, dc]) for dz, dy, dx, dc in ORDER]
    me = row * 8 + col

    pieces = [pl.ds(piece * PIECE, PIECE) for piece in range(128 // PIECE)]
    loads = []
    for at, piece in enumerate(pieces):
        loads.append((
            pltpu.make_async_copy(grad_ref.at[piece], grad.at[piece], loaded.at[0, at]),
            pltpu.make_async_copy(moment_ref.at[piece], moment.at[piece], loaded.at[1, at]),
        ))
    for pair in loads:
        for load in pair:
            load.start()
    weights = pltpu.make_async_copy(weight_ref, out_ref, held)
    weights.start()

    barrier = pltpu.get_barrier_semaphore()
    for place in places:
        pl.semaphore_signal(barrier, inc=1, device_id=place, device_id_type=MESH)
    for piece, pair in zip(pieces, loads):
        for load in pair:
            load.wait()
        x_ref[piece] = hold_rate * moment[piece] + grad[piece]
    pl.semaphore_wait(barrier, len(places))

    for stage in range(STAGES):
        pltpu.make_async_copy(x_ref.at[me, stage], taken.at[stage, row, col], got.at[stage]).start()
        for place in places:
            pltpu.make_async_remote_copy(
                src_ref=x_ref.at[place[0] * 8 + place[1], stage],
                dst_ref=taken.at[stage, row, col],
                send_sem=sent.at[stage],
                recv_sem=got.at[stage],
                device_id=place,
                device_id_type=MESH,
            ).start()

    up = lax.broadcasted_iota(jnp.int32, (128, 128), 0)
    across = lax.broadcasted_iota(jnp.int32, (128, 128), 1)
    same_half = (up // 4) % 2 == (across // 4) % 2
    upper = (across // 4) % 2 == 1
    eye = jnp.where(up == across, 1.0, 0.0).astype(jnp.float32)

    def gram_of(split):
        high, middle, low = split
        both = lax.dot_general(
            jnp.concatenate(split, axis=0), jnp.concatenate((high, middle), axis=0),
            (((1,), (1,)), ((), ())), preferred_element_type=jnp.float32,
        )
        last = both[256:, :128] + both[256:, 128:]
        mixed = both[:128, 128:] + both[128:256, :128]
        both = both[:128, :128] + (mixed + (both[128:256, 128:] + (last + last.T)))
        both = jnp.where(same_half, both, 0.0)
        other = pltpu.roll(both.reshape(16, 8, 128), 4, 1).reshape(128, 128)
        other = jnp.where(upper, pltpu.roll(other, 4, 1), pltpu.roll(other, 124, 1))
        return both + other

    for stage in range(STAGES):
        pltpu.make_async_copy(taken.at[stage], taken.at[stage], got.at[stage]).wait()
        wide = jnp.concatenate([taken[stage, :, c].reshape(128, 128) for c in range(8)], axis=1)
        split = parts(wide)
        gram = gram_of(split)
        total = 0.5 * jnp.sum(jnp.where(up == across, gram, 0.0), keepdims=True)
        scale = lax.rsqrt(total + 1e-06)
        mix = mixing(gram * (scale * scale), eye, 2) * scale
        split = parts(product(parts(mix), split))
        mix = mixing(gram_of(split), eye, 3)
        wide = product(parts(mix), split)
        for c in range(8):
            made[stage, :, c] = wide[:, c * 128 : c * 128 + 128].reshape(16, 8, 128)
        pltpu.make_async_copy(made.at[stage, row, col], landed.at[stage, me], back_got.at[stage]).start()
        for place in places:
            pltpu.make_async_remote_copy(
                src_ref=made.at[stage, place[0], place[1]],
                dst_ref=landed.at[stage, me],
                send_sem=back_sent.at[stage],
                recv_sem=back_got.at[stage],
                device_id=place,
                device_id_type=MESH,
            ).start()

    weights.wait()
    for stage in range(STAGES):
        pltpu.make_async_copy(landed.at[stage], landed.at[stage], back_got.at[stage]).wait()
        out_ref[:, stage] = out_ref[:, stage] - learn_rate * landed[stage]
    part = landed.at[0, pl.ds(0, 127)]
    for stage in range(STAGES):
        pltpu.make_async_copy(part, part, sent.at[stage]).wait()
        pltpu.make_async_copy(part, part, back_sent.at[stage]).wait()


def write_out(weights, momentum, weights_out, momentum_out, done):
    copies = [
        pltpu.make_async_copy(weights, weights_out, done.at[0]),
        pltpu.make_async_copy(momentum, momentum_out, done.at[1]),
    ]
    for copy in copies:
        copy.start()
    for copy in copies:
        copy.wait()


def to_tiles(array):
    return array.reshape(512, 4, 2, 128).transpose(0, 2, 1, 3).reshape(128, 4, 8, 128)


def from_tiles(array):
    return array.reshape(512, 2, 4, 128).transpose(0, 2, 1, 3).reshape(512, 4, 256)


def on_device(grad_stack, moment_stack, weight_stack):
    tiles = jax.ShapeDtypeStruct((128, 4, 8, 128), jnp.float32)
    in_vmem = pl.BlockSpec(memory_space=pltpu.VMEM)
    anywhere = pl.BlockSpec(memory_space=pl.ANY)
    updated = pl.pallas_call(
        kernel,
        out_shape=(tiles, tiles),
        in_specs=[anywhere] * 3,
        out_specs=[in_vmem] * 2,
        scratch_shapes=[
            pltpu.VMEM((128, 4, 8, 128), jnp.float32),
            pltpu.VMEM((128, 4, 8, 128), jnp.float32),
            pltpu.VMEM((STAGES, 16, 8, 8, 128), jnp.float32),
            pltpu.VMEM((STAGES, 16, 8, 8, 128), jnp.float32),
            pltpu.VMEM((STAGES, 128, 8, 128), jnp.float32),
            pltpu.SemaphoreType.DMA((STAGES,)),
            pltpu.SemaphoreType.DMA((STAGES,)),
            pltpu.SemaphoreType.DMA((STAGES,)),
            pltpu.SemaphoreType.DMA((STAGES,)),
            pltpu.SemaphoreType.DMA((2, 128 // PIECE)),
            pltpu.SemaphoreType.DMA,
        ],
        compiler_params=pltpu.CompilerParams(
            collective_id=1, has_side_effects=True, vmem_limit_bytes=48 * 1024 * 1024
        ),
    )(to_tiles(grad_stack), to_tiles(moment_stack), to_tiles(weight_stack))
    written = pl.pallas_call(
        write_out,
        out_shape=(tiles, tiles),
        in_specs=[in_vmem] * 2,
        out_specs=[anywhere] * 2,
        scratch_shapes=[pltpu.SemaphoreType.DMA((2,))],
        compiler_params=pltpu.CompilerParams(vmem_limit_bytes=16 * 1024 * 1024),
    )(*updated)
    return tuple(from_tiles(array) for array in written)


def solution(mesh):
    placed = (P(None, "rows", "cols"), P(None, "rows", "cols"), P(None, "rows", "cols"))
    return jax.shard_map(
        on_device,
        mesh=mesh,
        in_specs=placed,
        out_specs=(P(None, "rows", "cols"), P(None, "rows", "cols")),
        check_vma=False,
    )
```

```python
import itertools

import jax
import jax.numpy as jnp
from jax import lax
from jax.experimental import pallas as pl
from jax.experimental.pallas import tpu as pltpu
from jax.sharding import PartitionSpec as P

hold_rate = 0.95
learn_rate = 1.0
LINEAR, CUBIC, QUINTIC = 3.4445, -4.775, 2.0315

MESH = pl.DeviceIdType.MESH
STAGES = 4
PIECE = 16


def by_distance():
    levels = {}
    for core in range(2):
        for offset in itertools.product(range(4), repeat=3):
            if any(offset) or core:
                hops = max(1, sum(min(d, 4 - d) for d in offset))
                levels.setdefault(hops, []).append(offset + (core,))

    def twins(offset):
        opposite = tuple(-d % 4 for d in offset[:3])
        turn = sum(1 for d in offset[:3] if d == 2)
        return (turn, max(offset[:3], opposite), offset[3], offset)

    return [sorted(levels[hops], key=twins) for hops in sorted(levels)]


LEVELS = by_distance()
NEAR = 2


def parts(array):
    high = array.astype(jnp.bfloat16)
    rest = array - high.astype(jnp.float32)
    middle = rest.astype(jnp.bfloat16)
    return high, middle, (rest - middle.astype(jnp.float32)).astype(jnp.bfloat16)


def product(left, right):
    high, middle, low = left
    high_right, middle_right, low_right = right
    side = lambda *arrays: jnp.concatenate(arrays, axis=1)
    above = lambda *arrays: jnp.concatenate(arrays, axis=0)
    dot = lambda x, y: jnp.dot(x, y, preferred_element_type=jnp.float32)
    large = dot(above(side(high, high), side(middle, middle)), above(high_right, middle_right))
    small = dot(side(low, high), above(high_right, low_right))
    return large[:128] + (large[128:] + small)


def mixing(gram, eye, steps):
    mix = None
    for step in range(steps):
        split = parts(gram)
        poly = LINEAR * eye + CUBIC * gram + QUINTIC * product(split, split)
        split_poly = parts(poly)
        mix = poly if mix is None else product(split_poly, parts(mix))
        if step < steps - 1:
            gram = product(split_poly, parts(product(split_poly, split)))
    return mix


def kernel(
    grad_ref, moment_ref, weight_ref, out_ref, x_ref,
    grad, moment, taken, made, landed, sent, got, back_sent, back_got, loaded, held, near,
):
    row, col = lax.axis_index("rows"), lax.axis_index("cols")
    z, y, x, core = row // 4, row % 4, col // 2, col % 2
    zs = [lax.rem(z + d, 4) for d in range(4)]
    ys = [lax.rem(y + d, 4) for d in range(4)]
    xs = [lax.rem(x + d, 4) for d in range(4)]
    cores = [core, 1 - core]
    rows = {(a, b): zs[a] * 4 + ys[b] for a in range(4) for b in range(4)}
    cols = {(a, b): xs[a] * 2 + cores[b] for a in range(4) for b in range(2)}
    levels = [[(rows[dz, dy], cols[dx, dc]) for dz, dy, dx, dc in level] for level in LEVELS]
    me = row * 8 + col

    pieces = [pl.ds(piece * PIECE, PIECE) for piece in range(128 // PIECE)]
    loads = []
    for at, piece in enumerate(pieces):
        loads.append((
            pltpu.make_async_copy(grad_ref.at[piece], grad.at[piece], loaded.at[0, at]),
            pltpu.make_async_copy(moment_ref.at[piece], moment.at[piece], loaded.at[1, at]),
        ))
    for pair in loads:
        for load in pair:
            load.start()
    weights = pltpu.make_async_copy(weight_ref, out_ref, held)
    weights.start()

    def tell(semaphore):
        for place in levels[0]:
            pl.semaphore_signal(semaphore, inc=1, device_id=place, device_id_type=MESH)

    def hear(semaphore):
        pl.semaphore_wait(semaphore, len(levels[0]))

    def send(stage, level):
        for place in level:
            pltpu.make_async_remote_copy(
                src_ref=x_ref.at[place[0] * 8 + place[1], stage],
                dst_ref=taken.at[stage, row, col],
                send_sem=sent.at[stage],
                recv_sem=got.at[stage],
                device_id=place,
                device_id_type=MESH,
            ).start()

    tell(pltpu.get_barrier_semaphore())
    hear(pltpu.get_barrier_semaphore())
    tell(near.at[0])
    for piece, pair in zip(pieces, loads):
        for load in pair:
            load.wait()
        x_ref[piece] = hold_rate * moment[piece] + grad[piece]
    hear(near.at[0])
    tell(near.at[1])
    for stage in range(STAGES):
        pltpu.make_async_copy(x_ref.at[me, stage], taken.at[stage, row, col], got.at[stage]).start()
    for level in levels[:NEAR]:
        for stage in range(STAGES):
            send(stage, level)
    for hops in range(NEAR, len(levels)):
        hear(near.at[hops - 1])
        if hops < len(levels) - 1:
            tell(near.at[hops])
        send(0, levels[hops])
    for stage in range(1, STAGES):
        for level in levels[NEAR:]:
            send(stage, level)

    up = lax.broadcasted_iota(jnp.int32, (128, 128), 0)
    across = lax.broadcasted_iota(jnp.int32, (128, 128), 1)
    same_half = (up // 4) % 2 == (across // 4) % 2
    upper = (across // 4) % 2 == 1
    eye = jnp.where(up == across, 1.0, 0.0).astype(jnp.float32)

    def gram_of(split):
        high, middle, low = split
        both = lax.dot_general(
            jnp.concatenate(split, axis=0), jnp.concatenate((high, middle), axis=0),
            (((1,), (1,)), ((), ())), preferred_element_type=jnp.float32,
        )
        last = both[256:, :128] + both[256:, 128:]
        mixed = both[:128, 128:] + both[128:256, :128]
        both = both[:128, :128] + (mixed + (both[128:256, 128:] + (last + last.T)))
        both = jnp.where(same_half, both, 0.0)
        other = pltpu.roll(both.reshape(16, 8, 128), 4, 1).reshape(128, 128)
        other = jnp.where(upper, pltpu.roll(other, 4, 1), pltpu.roll(other, 124, 1))
        return both + other

    for stage in range(STAGES):
        pltpu.make_async_copy(taken.at[stage], taken.at[stage], got.at[stage]).wait()
        wide = jnp.concatenate([taken[stage, :, c].reshape(128, 128) for c in range(8)], axis=1)
        split = parts(wide)
        gram = gram_of(split)
        total = 0.5 * jnp.sum(jnp.where(up == across, gram, 0.0), keepdims=True)
        scale = lax.rsqrt(total + 1e-06)
        mix = mixing(gram * (scale * scale), eye, 2) * scale
        split = parts(product(parts(mix), split))
        mix = mixing(gram_of(split), eye, 3)
        wide = product(parts(mix), split)
        for c in range(8):
            made[stage, :, c] = wide[:, c * 128 : c * 128 + 128].reshape(16, 8, 128)
        pltpu.make_async_copy(made.at[stage, row, col], landed.at[stage, me], back_got.at[stage]).start()
        for place in itertools.chain(*reversed(levels)):
            pltpu.make_async_remote_copy(
                src_ref=made.at[stage, place[0], place[1]],
                dst_ref=landed.at[stage, me],
                send_sem=back_sent.at[stage],
                recv_sem=back_got.at[stage],
                device_id=place,
                device_id_type=MESH,
            ).start()

    weights.wait()
    for stage in range(STAGES):
        pltpu.make_async_copy(landed.at[stage], landed.at[stage], back_got.at[stage]).wait()
        out_ref[:, stage] = out_ref[:, stage] - learn_rate * landed[stage]
    part = landed.at[0, pl.ds(0, 127)]
    for stage in range(STAGES):
        pltpu.make_async_copy(part, part, sent.at[stage]).wait()
        pltpu.make_async_copy(part, part, back_sent.at[stage]).wait()


def write_out(weights, momentum, weights_out, momentum_out, done):
    copies = [
        pltpu.make_async_copy(weights, weights_out, done.at[0]),
        pltpu.make_async_copy(momentum, momentum_out, done.at[1]),
    ]
    for copy in copies:
        copy.start()
    for copy in copies:
        copy.wait()


def to_tiles(array):
    return array.reshape(512, 4, 2, 128).transpose(0, 2, 1, 3).reshape(128, 4, 8, 128)


def from_tiles(array):
    return array.reshape(512, 2, 4, 128).transpose(0, 2, 1, 3).reshape(512, 4, 256)


def on_device(grad_stack, moment_stack, weight_stack):
    tiles = jax.ShapeDtypeStruct((128, 4, 8, 128), jnp.float32)
    in_vmem = pl.BlockSpec(memory_space=pltpu.VMEM)
    anywhere = pl.BlockSpec(memory_space=pl.ANY)
    updated = pl.pallas_call(
        kernel,
        out_shape=(tiles, tiles),
        in_specs=[anywhere] * 3,
        out_specs=[in_vmem] * 2,
        scratch_shapes=[
            pltpu.VMEM((128, 4, 8, 128), jnp.float32),
            pltpu.VMEM((128, 4, 8, 128), jnp.float32),
            pltpu.VMEM((STAGES, 16, 8, 8, 128), jnp.float32),
            pltpu.VMEM((STAGES, 16, 8, 8, 128), jnp.float32),
            pltpu.VMEM((STAGES, 128, 8, 128), jnp.float32),
            pltpu.SemaphoreType.DMA((STAGES,)),
            pltpu.SemaphoreType.DMA((STAGES,)),
            pltpu.SemaphoreType.DMA((STAGES,)),
            pltpu.SemaphoreType.DMA((STAGES,)),
            pltpu.SemaphoreType.DMA((2, 128 // PIECE)),
            pltpu.SemaphoreType.DMA,
            pltpu.SemaphoreType.REGULAR((len(LEVELS) - 1,)),
        ],
        compiler_params=pltpu.CompilerParams(
            collective_id=1, has_side_effects=True, vmem_limit_bytes=48 * 1024 * 1024
        ),
    )(to_tiles(grad_stack), to_tiles(moment_stack), to_tiles(weight_stack))
    written = pl.pallas_call(
        write_out,
        out_shape=(tiles, tiles),
        in_specs=[in_vmem] * 2,
        out_specs=[anywhere] * 2,
        scratch_shapes=[pltpu.SemaphoreType.DMA((2,))],
        compiler_params=pltpu.CompilerParams(vmem_limit_bytes=16 * 1024 * 1024),
    )(*updated)
    return tuple(from_tiles(array) for array in written)


def solution(mesh):
    placed = (P(None, "rows", "cols"), P(None, "rows", "cols"), P(None, "rows", "cols"))
    return jax.shard_map(
        on_device,
        mesh=mesh,
        in_specs=placed,
        out_specs=(P(None, "rows", "cols"), P(None, "rows", "cols")),
        check_vma=False,
    )
```

```python
import itertools

import jax
import jax.numpy as jnp
from jax import lax
from jax.experimental import pallas as pl
from jax.experimental.pallas import tpu as pltpu
from jax.sharding import PartitionSpec as P

hold_rate = 0.95
learn_rate = 1.0
LINEAR, CUBIC, QUINTIC = 3.4445, -4.775, 2.0315

MESH = pl.DeviceIdType.MESH
STAGES = 4
PIECE = 16


def send_order():
    def put(axes, values):
        offset = [0, 0, 0]
        for axis, value in zip(axes, values):
            offset[axis] = value % 4
        return tuple(offset)

    rounds = [[(2, 2, 2)]]
    for a, b in itertools.product((1, -1), repeat=2):
        rounds.append([put((0, 1, 2), (1, a, b)), put((0, 1, 2), (-1, -a, -b))])
    for d in range(3):
        e, f = [axis for axis in range(3) if axis != d]
        for a, b in itertools.product((1, -1), repeat=2):
            rounds.append([put((d, e, f), (2, a, b)), put((d, e, f), (0, -a, -b))])
        for a in (1, -1):
            rounds.append([put((d, e, f), (a, 2, 2)), put((d, e, f), (-a, 0, 0))])
        rounds.append([put((d, e, f), (0, 2, 2)), put((d, e, f), (2, 0, 0))])
        for a in (1, -1):
            rounds.append([put((d, e, f), (a, 2, 0)), put((d, e, f), (-a, 0, 2))])
    order = [(0, 0, 0, 1)]
    for group in rounds:
        for core in range(2):
            order += [offset + (core,) for offset in group]
    assert len(set(order)) == 127
    return order


ORDER = send_order()


def parts(array):
    high = array.astype(jnp.bfloat16)
    rest = array - high.astype(jnp.float32)
    middle = rest.astype(jnp.bfloat16)
    return high, middle, (rest - middle.astype(jnp.float32)).astype(jnp.bfloat16)


def product(left, right):
    high, middle, low = left
    high_right, middle_right, low_right = right
    side = lambda *arrays: jnp.concatenate(arrays, axis=1)
    above = lambda *arrays: jnp.concatenate(arrays, axis=0)
    dot = lambda x, y: jnp.dot(x, y, preferred_element_type=jnp.float32)
    large = dot(above(side(high, high), side(middle, middle)), above(high_right, middle_right))
    small = dot(side(low, high), above(high_right, low_right))
    return large[:128] + (large[128:] + small)


def mixing(gram, eye, steps):
    mix = None
    for step in range(steps):
        split = parts(gram)
        poly = LINEAR * eye + CUBIC * gram + QUINTIC * product(split, split)
        split_poly = parts(poly)
        mix = poly if mix is None else product(split_poly, parts(mix))
        if step < steps - 1:
            gram = product(split_poly, parts(product(split_poly, split)))
    return mix


def kernel(
    grad_ref, moment_ref, weight_ref, out_ref, x_ref,
    grad, moment, taken, made, landed, sent, got, back_sent, back_got, loaded, held,
):
    row, col = lax.axis_index("rows"), lax.axis_index("cols")
    z, y, x, core = row // 4, row % 4, col // 2, col % 2
    zs = [lax.rem(z + d, 4) for d in range(4)]
    ys = [lax.rem(y + d, 4) for d in range(4)]
    xs = [lax.rem(x + d, 4) for d in range(4)]
    cores = [core, 1 - core]
    rows = {(a, b): zs[a] * 4 + ys[b] for a in range(4) for b in range(4)}
    cols = {(a, b): xs[a] * 2 + cores[b] for a in range(4) for b in range(2)}
    places = [(rows[dz, dy], cols[dx, dc]) for dz, dy, dx, dc in ORDER]
    me = row * 8 + col

    pieces = [pl.ds(piece * PIECE, PIECE) for piece in range(128 // PIECE)]
    loads = []
    for at, piece in enumerate(pieces):
        loads.append((
            pltpu.make_async_copy(grad_ref.at[piece], grad.at[piece], loaded.at[0, at]),
            pltpu.make_async_copy(moment_ref.at[piece], moment.at[piece], loaded.at[1, at]),
        ))
    for pair in loads:
        for load in pair:
            load.start()
    weights = pltpu.make_async_copy(weight_ref, out_ref, held)
    weights.start()

    with jax.named_scope("greet"):
        barrier = pltpu.get_barrier_semaphore()
        far = sorted(range(127), key=lambda at: -sum(min(d, 4 - d) for d in ORDER[at][:3]))
        for place in [places[at] for at in far]:
            pl.semaphore_signal(barrier, inc=1, device_id=place, device_id_type=MESH)
    with jax.named_scope("momentum"):
        for piece, pair in zip(pieces, loads):
            for load in pair:
                load.wait()
            x_ref[piece] = hold_rate * moment[piece] + grad[piece]
    with jax.named_scope("greetwait"):
        pl.semaphore_wait(barrier, len(places))

    for stage in range(STAGES):
        with jax.named_scope(f"fsend{stage}"):
            pltpu.make_async_copy(x_ref.at[me, stage], taken.at[stage, row, col], got.at[stage]).start()
            for place in places:
                pltpu.make_async_remote_copy(
                    src_ref=x_ref.at[place[0] * 8 + place[1], stage],
                    dst_ref=taken.at[stage, row, col],
                    send_sem=sent.at[stage],
                    recv_sem=got.at[stage],
                    device_id=place,
                    device_id_type=MESH,
                ).start()

    up = lax.broadcasted_iota(jnp.int32, (128, 128), 0)
    across = lax.broadcasted_iota(jnp.int32, (128, 128), 1)
    same_half = (up // 4) % 2 == (across // 4) % 2
    upper = (across // 4) % 2 == 1
    eye = jnp.where(up == across, 1.0, 0.0).astype(jnp.float32)

    def gram_of(split):
        high, middle, low = split
        both = lax.dot_general(
            jnp.concatenate(split, axis=0), jnp.concatenate((high, middle), axis=0),
            (((1,), (1,)), ((), ())), preferred_element_type=jnp.float32,
        )
        last = both[256:, :128] + both[256:, 128:]
        mixed = both[:128, 128:] + both[128:256, :128]
        both = both[:128, :128] + (mixed + (both[128:256, 128:] + (last + last.T)))
        both = jnp.where(same_half, both, 0.0)
        other = pltpu.roll(both.reshape(16, 8, 128), 4, 1).reshape(128, 128)
        other = jnp.where(upper, pltpu.roll(other, 4, 1), pltpu.roll(other, 124, 1))
        return both + other

    for stage in range(STAGES):
        with jax.named_scope(f"fwait{stage}"):
            pltpu.make_async_copy(taken.at[stage], taken.at[stage], got.at[stage]).wait()
        with jax.named_scope(f"comp{stage}"):
            wide = jnp.concatenate([taken[stage, :, c].reshape(128, 128) for c in range(8)], axis=1)
            split = parts(wide)
            gram = gram_of(split)
            total = 0.5 * jnp.sum(jnp.where(up == across, gram, 0.0), keepdims=True)
            scale = lax.rsqrt(total + 1e-06)
            mix = mixing(gram * (scale * scale), eye, 2) * scale
            split = parts(product(parts(mix), split))
            mix = mixing(gram_of(split), eye, 3)
            wide = product(parts(mix), split)
            for c in range(8):
                made[stage, :, c] = wide[:, c * 128 : c * 128 + 128].reshape(16, 8, 128)
        with jax.named_scope(f"bsend{stage}"):
            pltpu.make_async_copy(made.at[stage, row, col], landed.at[stage, me], back_got.at[stage]).start()
            for place in places[::-1]:
                pltpu.make_async_remote_copy(
                    src_ref=made.at[stage, place[0], place[1]],
                    dst_ref=landed.at[stage, me],
                    send_sem=back_sent.at[stage],
                    recv_sem=back_got.at[stage],
                    device_id=place,
                    device_id_type=MESH,
                ).start()

    weights.wait()
    for stage in range(STAGES):
        with jax.named_scope(f"bwait{stage}"):
            pltpu.make_async_copy(landed.at[stage], landed.at[stage], back_got.at[stage]).wait()
        out_ref[:, stage] = out_ref[:, stage] - learn_rate * landed[stage]
    with jax.named_scope("drain"):
        part = landed.at[0, pl.ds(0, 127)]
        for stage in range(STAGES):
            pltpu.make_async_copy(part, part, sent.at[stage]).wait()
            pltpu.make_async_copy(part, part, back_sent.at[stage]).wait()


def write_out(weights, momentum, weights_out, momentum_out, done):
    copies = [
        pltpu.make_async_copy(weights, weights_out, done.at[0]),
        pltpu.make_async_copy(momentum, momentum_out, done.at[1]),
    ]
    for copy in copies:
        copy.start()
    for copy in copies:
        copy.wait()


def to_tiles(array):
    return array.reshape(512, 4, 2, 128).transpose(0, 2, 1, 3).reshape(128, 4, 8, 128)


def from_tiles(array):
    return array.reshape(512, 2, 4, 128).transpose(0, 2, 1, 3).reshape(512, 4, 256)


def on_device(grad_stack, moment_stack, weight_stack):
    tiles = jax.ShapeDtypeStruct((128, 4, 8, 128), jnp.float32)
    in_vmem = pl.BlockSpec(memory_space=pltpu.VMEM)
    anywhere = pl.BlockSpec(memory_space=pl.ANY)
    updated = pl.pallas_call(
        kernel,
        out_shape=(tiles, tiles),
        in_specs=[anywhere] * 3,
        out_specs=[in_vmem] * 2,
        scratch_shapes=[
            pltpu.VMEM((128, 4, 8, 128), jnp.float32),
            pltpu.VMEM((128, 4, 8, 128), jnp.float32),
            pltpu.VMEM((STAGES, 16, 8, 8, 128), jnp.float32),
            pltpu.VMEM((STAGES, 16, 8, 8, 128), jnp.float32),
            pltpu.VMEM((STAGES, 128, 8, 128), jnp.float32),
            pltpu.SemaphoreType.DMA((STAGES,)),
            pltpu.SemaphoreType.DMA((STAGES,)),
            pltpu.SemaphoreType.DMA((STAGES,)),
            pltpu.SemaphoreType.DMA((STAGES,)),
            pltpu.SemaphoreType.DMA((2, 128 // PIECE)),
            pltpu.SemaphoreType.DMA,
        ],
        compiler_params=pltpu.CompilerParams(
            collective_id=1, has_side_effects=True, vmem_limit_bytes=48 * 1024 * 1024
        ),
    )(to_tiles(grad_stack), to_tiles(moment_stack), to_tiles(weight_stack))
    written = pl.pallas_call(
        write_out,
        out_shape=(tiles, tiles),
        in_specs=[in_vmem] * 2,
        out_specs=[anywhere] * 2,
        scratch_shapes=[pltpu.SemaphoreType.DMA((2,))],
        compiler_params=pltpu.CompilerParams(vmem_limit_bytes=16 * 1024 * 1024),
    )(*updated)
    return tuple(from_tiles(array) for array in written)


def solution(mesh):
    placed = (P(None, "rows", "cols"), P(None, "rows", "cols"), P(None, "rows", "cols"))
    return jax.shard_map(
        on_device,
        mesh=mesh,
        in_specs=placed,
        out_specs=(P(None, "rows", "cols"), P(None, "rows", "cols")),
        check_vma=False,
    )
```

```python
import itertools

import jax
import jax.numpy as jnp
from jax import lax
from jax.experimental import pallas as pl
from jax.experimental.pallas import tpu as pltpu
from jax.sharding import PartitionSpec as P

hold_rate = 0.95
learn_rate = 1.0
LINEAR, CUBIC, QUINTIC = 3.4445, -4.775, 2.0315

MESH = pl.DeviceIdType.MESH
STAGES = 4
PIECE = 16


def send_order():
    def put(axes, values):
        offset = [0, 0, 0]
        for axis, value in zip(axes, values):
            offset[axis] = value % 4
        return tuple(offset)

    rounds = [[(2, 2, 2)]]
    for a, b in itertools.product((1, -1), repeat=2):
        rounds.append([put((0, 1, 2), (1, a, b)), put((0, 1, 2), (-1, -a, -b))])
    for d in range(3):
        e, f = [axis for axis in range(3) if axis != d]
        for a, b in itertools.product((1, -1), repeat=2):
            rounds.append([put((d, e, f), (2, a, b)), put((d, e, f), (0, -a, -b))])
        for a in (1, -1):
            rounds.append([put((d, e, f), (a, 2, 2)), put((d, e, f), (-a, 0, 0))])
        rounds.append([put((d, e, f), (0, 2, 2)), put((d, e, f), (2, 0, 0))])
        for a in (1, -1):
            rounds.append([put((d, e, f), (a, 2, 0)), put((d, e, f), (-a, 0, 2))])
    order = [(0, 0, 0, 1)]
    for group in rounds:
        for core in range(2):
            order += [offset + (core,) for offset in group]
    assert len(set(order)) == 127
    return order


ORDER = send_order()


def parts(array):
    high = array.astype(jnp.bfloat16)
    rest = array - high.astype(jnp.float32)
    middle = rest.astype(jnp.bfloat16)
    return high, middle, (rest - middle.astype(jnp.float32)).astype(jnp.bfloat16)


def product(left, right):
    high, middle, low = left
    high_right, middle_right, low_right = right
    side = lambda *arrays: jnp.concatenate(arrays, axis=1)
    above = lambda *arrays: jnp.concatenate(arrays, axis=0)
    dot = lambda x, y: jnp.dot(x, y, preferred_element_type=jnp.float32)
    large = dot(above(side(high, high), side(middle, middle)), above(high_right, middle_right))
    small = dot(side(low, high), above(high_right, low_right))
    return large[:128] + (large[128:] + small)


def mixing(gram, eye, steps):
    mix = None
    for step in range(steps):
        split = parts(gram)
        poly = LINEAR * eye + CUBIC * gram + QUINTIC * product(split, split)
        split_poly = parts(poly)
        mix = poly if mix is None else product(split_poly, parts(mix))
        if step < steps - 1:
            gram = product(split_poly, parts(product(split_poly, split)))
    return mix


def kernel(
    grad_ref, moment_ref, weight_ref, out_ref, x_ref,
    grad, moment, taken, made, landed, sent, got, back_sent, back_got, loaded, held,
):
    row, col = lax.axis_index("rows"), lax.axis_index("cols")
    z, y, x, core = row // 4, row % 4, col // 2, col % 2
    zs = [lax.rem(z + d, 4) for d in range(4)]
    ys = [lax.rem(y + d, 4) for d in range(4)]
    xs = [lax.rem(x + d, 4) for d in range(4)]
    cores = [core, 1 - core]
    rows = {(a, b): zs[a] * 4 + ys[b] for a in range(4) for b in range(4)}
    cols = {(a, b): xs[a] * 2 + cores[b] for a in range(4) for b in range(2)}
    places = [(rows[dz, dy], cols[dx, dc]) for dz, dy, dx, dc in ORDER]
    me = row * 8 + col

    pieces = [pl.ds(piece * PIECE, PIECE) for piece in range(128 // PIECE)]
    loads = []
    for at, piece in enumerate(pieces):
        loads.append((
            pltpu.make_async_copy(grad_ref.at[piece], grad.at[piece], loaded.at[0, at]),
            pltpu.make_async_copy(moment_ref.at[piece], moment.at[piece], loaded.at[1, at]),
        ))
    for pair in loads:
        for load in pair:
            load.start()
    weights = pltpu.make_async_copy(weight_ref, out_ref, held)

    with jax.named_scope("greet"):
        barrier = pltpu.get_barrier_semaphore()
        far = sorted(range(127), key=lambda at: -sum(min(d, 4 - d) for d in ORDER[at][:3]))
        for place in [places[at] for at in far]:
            pl.semaphore_signal(barrier, inc=1, device_id=place, device_id_type=MESH)
    with jax.named_scope("momentum"):
        for piece, pair in zip(pieces, loads):
            for load in pair:
                load.wait()
            x_ref[piece] = hold_rate * moment[piece] + grad[piece]
    with jax.named_scope("greetwait"):
        pl.semaphore_wait(barrier, len(places))

    for stage in range(STAGES):
        with jax.named_scope(f"fsend{stage}"):
            pltpu.make_async_copy(x_ref.at[me, stage], taken.at[stage, row, col], got.at[stage]).start()
            for place in places:
                pltpu.make_async_remote_copy(
                    src_ref=x_ref.at[place[0] * 8 + place[1], stage],
                    dst_ref=taken.at[stage, row, col],
                    send_sem=sent.at[stage],
                    recv_sem=got.at[stage],
                    device_id=place,
                    device_id_type=MESH,
                ).start()

    weights.start()

    up = lax.broadcasted_iota(jnp.int32, (128, 128), 0)
    across = lax.broadcasted_iota(jnp.int32, (128, 128), 1)
    same_half = (up // 4) % 2 == (across // 4) % 2
    upper = (across // 4) % 2 == 1
    eye = jnp.where(up == across, 1.0, 0.0).astype(jnp.float32)

    def gram_of(split):
        high, middle, low = split
        both = lax.dot_general(
            jnp.concatenate(split, axis=0), jnp.concatenate((high, middle), axis=0),
            (((1,), (1,)), ((), ())), preferred_element_type=jnp.float32,
        )
        last = both[256:, :128] + both[256:, 128:]
        mixed = both[:128, 128:] + both[128:256, :128]
        both = both[:128, :128] + (mixed + (both[128:256, 128:] + (last + last.T)))
        both = jnp.where(same_half, both, 0.0)
        other = pltpu.roll(both.reshape(16, 8, 128), 4, 1).reshape(128, 128)
        other = jnp.where(upper, pltpu.roll(other, 4, 1), pltpu.roll(other, 124, 1))
        return both + other

    for stage in range(STAGES):
        with jax.named_scope(f"fwait{stage}"):
            pltpu.make_async_copy(taken.at[stage], taken.at[stage], got.at[stage]).wait()
        with jax.named_scope(f"comp{stage}"):
            wide = jnp.concatenate([taken[stage, :, c].reshape(128, 128) for c in range(8)], axis=1)
            split = parts(wide)
            gram = gram_of(split)
            total = 0.5 * jnp.sum(jnp.where(up == across, gram, 0.0), keepdims=True)
            scale = lax.rsqrt(total + 1e-06)
            mix = mixing(gram * (scale * scale), eye, 2) * scale
            split = parts(product(parts(mix), split))
            mix = mixing(gram_of(split), eye, 3)
            wide = product(parts(mix), split)
            for c in range(8):
                made[stage, :, c] = wide[:, c * 128 : c * 128 + 128].reshape(16, 8, 128)
        with jax.named_scope(f"bsend{stage}"):
            pltpu.make_async_copy(made.at[stage, row, col], landed.at[stage, me], back_got.at[stage]).start()
            for place in places[::-1]:
                pltpu.make_async_remote_copy(
                    src_ref=made.at[stage, place[0], place[1]],
                    dst_ref=landed.at[stage, me],
                    send_sem=back_sent.at[stage],
                    recv_sem=back_got.at[stage],
                    device_id=place,
                    device_id_type=MESH,
                ).start()

    weights.wait()
    for stage in range(STAGES):
        with jax.named_scope(f"bwait{stage}"):
            pltpu.make_async_copy(landed.at[stage], landed.at[stage], back_got.at[stage]).wait()
        out_ref[:, stage] = out_ref[:, stage] - learn_rate * landed[stage]
    with jax.named_scope("drain"):
        part = landed.at[0, pl.ds(0, 127)]
        for stage in range(STAGES):
            pltpu.make_async_copy(part, part, sent.at[stage]).wait()
            pltpu.make_async_copy(part, part, back_sent.at[stage]).wait()


def write_out(weights, momentum, weights_out, momentum_out, done):
    copies = []
    for quarter in range(4):
        part = pl.ds(quarter * 32, 32)
        copies.append(pltpu.make_async_copy(weights.at[part], weights_out.at[part], done.at[0, quarter]))
        copies.append(pltpu.make_async_copy(momentum.at[part], momentum_out.at[part], done.at[1, quarter]))
    for copy in copies:
        copy.start()
    for copy in copies:
        copy.wait()


def to_tiles(array):
    return array.reshape(512, 4, 2, 128).transpose(0, 2, 1, 3).reshape(128, 4, 8, 128)


def from_tiles(array):
    return array.reshape(512, 2, 4, 128).transpose(0, 2, 1, 3).reshape(512, 4, 256)


def on_device(grad_stack, moment_stack, weight_stack):
    tiles = jax.ShapeDtypeStruct((128, 4, 8, 128), jnp.float32)
    in_vmem = pl.BlockSpec(memory_space=pltpu.VMEM)
    anywhere = pl.BlockSpec(memory_space=pl.ANY)
    updated = pl.pallas_call(
        kernel,
        out_shape=(tiles, tiles),
        in_specs=[anywhere] * 3,
        out_specs=[in_vmem] * 2,
        scratch_shapes=[
            pltpu.VMEM((128, 4, 8, 128), jnp.float32),
            pltpu.VMEM((128, 4, 8, 128), jnp.float32),
            pltpu.VMEM((STAGES, 16, 8, 8, 128), jnp.float32),
            pltpu.VMEM((STAGES, 16, 8, 8, 128), jnp.float32),
            pltpu.VMEM((STAGES, 128, 8, 128), jnp.float32),
            pltpu.SemaphoreType.DMA((STAGES,)),
            pltpu.SemaphoreType.DMA((STAGES,)),
            pltpu.SemaphoreType.DMA((STAGES,)),
            pltpu.SemaphoreType.DMA((STAGES,)),
            pltpu.SemaphoreType.DMA((2, 128 // PIECE)),
            pltpu.SemaphoreType.DMA,
        ],
        compiler_params=pltpu.CompilerParams(
            collective_id=1, has_side_effects=True, vmem_limit_bytes=48 * 1024 * 1024
        ),
    )(to_tiles(grad_stack), to_tiles(moment_stack), to_tiles(weight_stack))
    written = pl.pallas_call(
        write_out,
        out_shape=(tiles, tiles),
        in_specs=[in_vmem] * 2,
        out_specs=[anywhere] * 2,
        scratch_shapes=[pltpu.SemaphoreType.DMA((2, 4))],
        compiler_params=pltpu.CompilerParams(vmem_limit_bytes=16 * 1024 * 1024),
    )(*updated)
    return tuple(from_tiles(array) for array in written)


def solution(mesh):
    placed = (P(None, "rows", "cols"), P(None, "rows", "cols"), P(None, "rows", "cols"))
    return jax.shard_map(
        on_device,
        mesh=mesh,
        in_specs=placed,
        out_specs=(P(None, "rows", "cols"), P(None, "rows", "cols")),
        check_vma=False,
    )
```

```python
import itertools

import jax
import jax.numpy as jnp
from jax import lax
from jax.experimental import pallas as pl
from jax.experimental.pallas import tpu as pltpu
from jax.sharding import PartitionSpec as P

hold_rate = 0.95
learn_rate = 1.0
LINEAR, CUBIC, QUINTIC = 3.4445, -4.775, 2.0315

MESH = pl.DeviceIdType.MESH
STAGES = 4
PIECE = 16


def send_order():
    def put(axes, values):
        offset = [0, 0, 0]
        for axis, value in zip(axes, values):
            offset[axis] = value % 4
        return tuple(offset)

    rounds = [[(2, 2, 2)]]
    for a, b in itertools.product((1, -1), repeat=2):
        rounds.append([put((0, 1, 2), (1, a, b)), put((0, 1, 2), (-1, -a, -b))])
    for d in range(3):
        e, f = [axis for axis in range(3) if axis != d]
        for a, b in itertools.product((1, -1), repeat=2):
            rounds.append([put((d, e, f), (2, a, b)), put((d, e, f), (0, -a, -b))])
        for a in (1, -1):
            rounds.append([put((d, e, f), (a, 2, 2)), put((d, e, f), (-a, 0, 0))])
        rounds.append([put((d, e, f), (0, 2, 2)), put((d, e, f), (2, 0, 0))])
        for a in (1, -1):
            rounds.append([put((d, e, f), (a, 2, 0)), put((d, e, f), (-a, 0, 2))])
    order = [(0, 0, 0, 1)]
    for group in rounds:
        for core in range(2):
            order += [offset + (core,) for offset in group]
    assert len(set(order)) == 127
    return order


ORDER = send_order()


def parts(array):
    high = array.astype(jnp.bfloat16)
    rest = array - high.astype(jnp.float32)
    middle = rest.astype(jnp.bfloat16)
    return high, middle, (rest - middle.astype(jnp.float32)).astype(jnp.bfloat16)


def product(left, right):
    high, middle, low = left
    high_right, middle_right, low_right = right
    side = lambda *arrays: jnp.concatenate(arrays, axis=1)
    above = lambda *arrays: jnp.concatenate(arrays, axis=0)
    dot = lambda x, y: jnp.dot(x, y, preferred_element_type=jnp.float32)
    large = dot(above(side(high, high), side(middle, middle)), above(high_right, middle_right))
    small = dot(side(low, high), above(high_right, low_right))
    return large[:128] + (large[128:] + small)


def mixing(gram, eye, steps):
    mix = None
    for step in range(steps):
        split = parts(gram)
        poly = LINEAR * eye + CUBIC * gram + QUINTIC * product(split, split)
        split_poly = parts(poly)
        mix = poly if mix is None else product(split_poly, parts(mix))
        if step < steps - 1:
            gram = product(split_poly, parts(product(split_poly, split)))
    return mix


def kernel(
    grad_ref, moment_ref, weight_ref, out_ref, x_ref,
    grad, moment, taken, made, landed, sent, got, back_sent, back_got, loaded, held,
):
    row, col = lax.axis_index("rows"), lax.axis_index("cols")
    z, y, x, core = row // 4, row % 4, col // 2, col % 2
    zs = [lax.rem(z + d, 4) for d in range(4)]
    ys = [lax.rem(y + d, 4) for d in range(4)]
    xs = [lax.rem(x + d, 4) for d in range(4)]
    cores = [core, 1 - core]
    rows = {(a, b): zs[a] * 4 + ys[b] for a in range(4) for b in range(4)}
    cols = {(a, b): xs[a] * 2 + cores[b] for a in range(4) for b in range(2)}
    places = [(rows[dz, dy], cols[dx, dc]) for dz, dy, dx, dc in ORDER]
    me = row * 8 + col

    pieces = [pl.ds(piece * PIECE, PIECE) for piece in range(128 // PIECE)]
    loads = []
    for at, piece in enumerate(pieces):
        loads.append((
            pltpu.make_async_copy(grad_ref.at[piece], grad.at[piece], loaded.at[0, at]),
            pltpu.make_async_copy(moment_ref.at[piece], moment.at[piece], loaded.at[1, at]),
        ))
    for pair in loads:
        for load in pair:
            load.start()
    weights = pltpu.make_async_copy(weight_ref, out_ref, held)
    weights.start()

    with jax.named_scope("greet"):
        barrier = pltpu.get_barrier_semaphore()
        far = sorted(range(127), key=lambda at: -sum(min(d, 4 - d) for d in ORDER[at][:3]))
        for place in [places[at] for at in far]:
            pl.semaphore_signal(barrier, inc=1, device_id=place, device_id_type=MESH)
    with jax.named_scope("momentum"):
        for piece, pair in zip(pieces, loads):
            for load in pair:
                load.wait()
            x_ref[piece] = hold_rate * moment[piece] + grad[piece]
    with jax.named_scope("greetwait"):
        pl.semaphore_wait(barrier, len(places))

    for stage in range(STAGES):
        with jax.named_scope(f"fsend{stage}"):
            pltpu.make_async_copy(x_ref.at[me, stage], taken.at[stage, row, col], got.at[stage]).start()
            for place in places:
                pltpu.make_async_remote_copy(
                    src_ref=x_ref.at[place[0] * 8 + place[1], stage],
                    dst_ref=taken.at[stage, row, col],
                    send_sem=sent.at[stage],
                    recv_sem=got.at[stage],
                    device_id=place,
                    device_id_type=MESH,
                ).start()

    up = lax.broadcasted_iota(jnp.int32, (128, 128), 0)
    across = lax.broadcasted_iota(jnp.int32, (128, 128), 1)
    same_half = (up // 4) % 2 == (across // 4) % 2
    upper = (across // 4) % 2 == 1
    eye = jnp.where(up == across, 1.0, 0.0).astype(jnp.float32)

    def gram_of(split):
        high, middle, low = split
        both = lax.dot_general(
            jnp.concatenate(split, axis=0), jnp.concatenate((high, middle), axis=0),
            (((1,), (1,)), ((), ())), preferred_element_type=jnp.float32,
        )
        last = both[256:, :128] + both[256:, 128:]
        mixed = both[:128, 128:] + both[128:256, :128]
        both = both[:128, :128] + (mixed + (both[128:256, 128:] + (last + last.T)))
        both = jnp.where(same_half, both, 0.0)
        other = pltpu.roll(both.reshape(16, 8, 128), 4, 1).reshape(128, 128)
        other = jnp.where(upper, pltpu.roll(other, 4, 1), pltpu.roll(other, 124, 1))
        return both + other

    def finish(stage, carry):
        with jax.named_scope("fwait"):
            pltpu.make_async_copy(taken.at[stage], taken.at[stage], got.at[stage]).wait()
        with jax.named_scope("comp"):
            wide = jnp.concatenate([taken[stage, :, c].reshape(128, 128) for c in range(8)], axis=1)
            split = parts(wide)
            gram = gram_of(split)
            total = 0.5 * jnp.sum(jnp.where(up == across, gram, 0.0), keepdims=True)
            scale = lax.rsqrt(total + 1e-06)
            mix = mixing(gram * (scale * scale), eye, 2) * scale
            split = parts(product(parts(mix), split))
            mix = mixing(gram_of(split), eye, 3)
            wide = product(parts(mix), split)
            for c in range(8):
                made[stage, :, c] = wide[:, c * 128 : c * 128 + 128].reshape(16, 8, 128)
        with jax.named_scope("bsend"):
            pltpu.make_async_copy(made.at[stage, row, col], landed.at[stage, me], back_got.at[stage]).start()
            for place in places[::-1]:
                pltpu.make_async_remote_copy(
                    src_ref=made.at[stage, place[0], place[1]],
                    dst_ref=landed.at[stage, me],
                    send_sem=back_sent.at[stage],
                    recv_sem=back_got.at[stage],
                    device_id=place,
                    device_id_type=MESH,
                ).start()
        return carry

    lax.fori_loop(0, STAGES, finish, 0)

    weights.wait()
    for stage in range(STAGES):
        with jax.named_scope(f"bwait{stage}"):
            pltpu.make_async_copy(landed.at[stage], landed.at[stage], back_got.at[stage]).wait()
        out_ref[:, stage] = out_ref[:, stage] - learn_rate * landed[stage]
    with jax.named_scope("drain"):
        part = landed.at[0, pl.ds(0, 127)]
        for stage in range(STAGES):
            pltpu.make_async_copy(part, part, sent.at[stage]).wait()
            pltpu.make_async_copy(part, part, back_sent.at[stage]).wait()


def write_out(weights, momentum, weights_out, momentum_out, done):
    copies = [
        pltpu.make_async_copy(weights, weights_out, done.at[0]),
        pltpu.make_async_copy(momentum, momentum_out, done.at[1]),
    ]
    for copy in copies:
        copy.start()
    for copy in copies:
        copy.wait()


def to_tiles(array):
    return array.reshape(512, 4, 2, 128).transpose(0, 2, 1, 3).reshape(128, 4, 8, 128)


def from_tiles(array):
    return array.reshape(512, 2, 4, 128).transpose(0, 2, 1, 3).reshape(512, 4, 256)


def on_device(grad_stack, moment_stack, weight_stack):
    tiles = jax.ShapeDtypeStruct((128, 4, 8, 128), jnp.float32)
    in_vmem = pl.BlockSpec(memory_space=pltpu.VMEM)
    anywhere = pl.BlockSpec(memory_space=pl.ANY)
    updated = pl.pallas_call(
        kernel,
        out_shape=(tiles, tiles),
        in_specs=[anywhere] * 3,
        out_specs=[in_vmem] * 2,
        scratch_shapes=[
            pltpu.VMEM((128, 4, 8, 128), jnp.float32),
            pltpu.VMEM((128, 4, 8, 128), jnp.float32),
            pltpu.VMEM((STAGES, 16, 8, 8, 128), jnp.float32),
            pltpu.VMEM((STAGES, 16, 8, 8, 128), jnp.float32),
            pltpu.VMEM((STAGES, 128, 8, 128), jnp.float32),
            pltpu.SemaphoreType.DMA((STAGES,)),
            pltpu.SemaphoreType.DMA((STAGES,)),
            pltpu.SemaphoreType.DMA((STAGES,)),
            pltpu.SemaphoreType.DMA((STAGES,)),
            pltpu.SemaphoreType.DMA((2, 128 // PIECE)),
            pltpu.SemaphoreType.DMA,
        ],
        compiler_params=pltpu.CompilerParams(
            collective_id=1, has_side_effects=True, vmem_limit_bytes=48 * 1024 * 1024
        ),
    )(to_tiles(grad_stack), to_tiles(moment_stack), to_tiles(weight_stack))
    written = pl.pallas_call(
        write_out,
        out_shape=(tiles, tiles),
        in_specs=[in_vmem] * 2,
        out_specs=[anywhere] * 2,
        scratch_shapes=[pltpu.SemaphoreType.DMA((2,))],
        compiler_params=pltpu.CompilerParams(vmem_limit_bytes=16 * 1024 * 1024),
    )(*updated)
    return tuple(from_tiles(array) for array in written)


def solution(mesh):
    placed = (P(None, "rows", "cols"), P(None, "rows", "cols"), P(None, "rows", "cols"))
    return jax.shard_map(
        on_device,
        mesh=mesh,
        in_specs=placed,
        out_specs=(P(None, "rows", "cols"), P(None, "rows", "cols")),
        check_vma=False,
    )
```

```python
import itertools

import jax
import jax.numpy as jnp
from jax import lax
from jax.experimental import pallas as pl
from jax.experimental.pallas import tpu as pltpu
from jax.sharding import PartitionSpec as P

hold_rate = 0.95
learn_rate = 1.0
LINEAR, CUBIC, QUINTIC = 3.4445, -4.775, 2.0315

MESH = pl.DeviceIdType.MESH
STAGES = 4
PIECE = 16


def send_order():
    def put(axes, values):
        offset = [0, 0, 0]
        for axis, value in zip(axes, values):
            offset[axis] = value % 4
        return tuple(offset)

    rounds = [[(2, 2, 2)]]
    for a, b in itertools.product((1, -1), repeat=2):
        rounds.append([put((0, 1, 2), (1, a, b)), put((0, 1, 2), (-1, -a, -b))])
    for d in range(3):
        e, f = [axis for axis in range(3) if axis != d]
        for a, b in itertools.product((1, -1), repeat=2):
            rounds.append([put((d, e, f), (2, a, b)), put((d, e, f), (0, -a, -b))])
        for a in (1, -1):
            rounds.append([put((d, e, f), (a, 2, 2)), put((d, e, f), (-a, 0, 0))])
        rounds.append([put((d, e, f), (0, 2, 2)), put((d, e, f), (2, 0, 0))])
        for a in (1, -1):
            rounds.append([put((d, e, f), (a, 2, 0)), put((d, e, f), (-a, 0, 2))])
    order = [(0, 0, 0, 1)]
    for group in rounds:
        for core in range(2):
            order += [offset + (core,) for offset in group]
    assert len(set(order)) == 127
    return order


ORDER = send_order()


def parts(array):
    high = array.astype(jnp.bfloat16)
    rest = array - high.astype(jnp.float32)
    middle = rest.astype(jnp.bfloat16)
    return high, middle, (rest - middle.astype(jnp.float32)).astype(jnp.bfloat16)


def product(left, right):
    high, middle, low = left
    high_right, middle_right, low_right = right
    side = lambda *arrays: jnp.concatenate(arrays, axis=1)
    above = lambda *arrays: jnp.concatenate(arrays, axis=0)
    dot = lambda x, y: jnp.dot(x, y, preferred_element_type=jnp.float32)
    large = dot(above(side(high, high), side(middle, middle)), above(high_right, middle_right))
    small = dot(side(low, high), above(high_right, low_right))
    return large[:128] + (large[128:] + small)


def mixing(grams, eye, steps):
    mixes = None
    for step in range(steps):
        splits = [parts(gram) for gram in grams]
        squares = [product(split, split) for split in splits]
        polys = [LINEAR * eye + CUBIC * gram + QUINTIC * square for gram, square in zip(grams, squares)]
        split_polys = [parts(poly) for poly in polys]
        if step < steps - 1:
            halfway = [parts(product(poly, split)) for poly, split in zip(split_polys, splits)]
        if mixes is None:
            mixes = polys
        else:
            mixes = [product(poly, parts(mix)) for poly, mix in zip(split_polys, mixes)]
        if step < steps - 1:
            grams = [product(poly, half) for poly, half in zip(split_polys, halfway)]
    return mixes


def kernel(
    grad_ref, moment_ref, weight_ref, out_ref, x_ref,
    grad, moment, taken, made, landed, sent, got, back_sent, back_got, loaded, held,
):
    row, col = lax.axis_index("rows"), lax.axis_index("cols")
    z, y, x, core = row // 4, row % 4, col // 2, col % 2
    zs = [lax.rem(z + d, 4) for d in range(4)]
    ys = [lax.rem(y + d, 4) for d in range(4)]
    xs = [lax.rem(x + d, 4) for d in range(4)]
    cores = [core, 1 - core]
    rows = {(a, b): zs[a] * 4 + ys[b] for a in range(4) for b in range(4)}
    cols = {(a, b): xs[a] * 2 + cores[b] for a in range(4) for b in range(2)}
    places = [(rows[dz, dy], cols[dx, dc]) for dz, dy, dx, dc in ORDER]
    me = row * 8 + col

    pieces = [pl.ds(piece * PIECE, PIECE) for piece in range(128 // PIECE)]
    loads = []
    for at, piece in enumerate(pieces):
        loads.append((
            pltpu.make_async_copy(grad_ref.at[piece], grad.at[piece], loaded.at[0, at]),
            pltpu.make_async_copy(moment_ref.at[piece], moment.at[piece], loaded.at[1, at]),
        ))
    for pair in loads:
        for load in pair:
            load.start()
    weights = pltpu.make_async_copy(weight_ref, out_ref, held)
    weights.start()

    with jax.named_scope("greet"):
        barrier = pltpu.get_barrier_semaphore()
        far = sorted(range(127), key=lambda at: -sum(min(d, 4 - d) for d in ORDER[at][:3]))
        for place in [places[at] for at in far]:
            pl.semaphore_signal(barrier, inc=1, device_id=place, device_id_type=MESH)
    with jax.named_scope("momentum"):
        for piece, pair in zip(pieces, loads):
            for load in pair:
                load.wait()
            x_ref[piece] = hold_rate * moment[piece] + grad[piece]
    with jax.named_scope("greetwait"):
        pl.semaphore_wait(barrier, len(places))

    for stage in range(STAGES):
        with jax.named_scope(f"fsend{stage}"):
            pltpu.make_async_copy(x_ref.at[me, stage], taken.at[stage, row, col], got.at[stage]).start()
            for place in places:
                pltpu.make_async_remote_copy(
                    src_ref=x_ref.at[place[0] * 8 + place[1], stage],
                    dst_ref=taken.at[stage, row, col],
                    send_sem=sent.at[stage],
                    recv_sem=got.at[stage],
                    device_id=place,
                    device_id_type=MESH,
                ).start()

    up = lax.broadcasted_iota(jnp.int32, (128, 128), 0)
    across = lax.broadcasted_iota(jnp.int32, (128, 128), 1)
    same_half = (up // 4) % 2 == (across // 4) % 2
    upper = (across // 4) % 2 == 1
    eye = jnp.where(up == across, 1.0, 0.0).astype(jnp.float32)

    def gram_of(split):
        high, middle, low = split
        both = lax.dot_general(
            jnp.concatenate(split, axis=0), jnp.concatenate((high, middle), axis=0),
            (((1,), (1,)), ((), ())), preferred_element_type=jnp.float32,
        )
        last = both[256:, :128] + both[256:, 128:]
        mixed = both[:128, 128:] + both[128:256, :128]
        both = both[:128, :128] + (mixed + (both[128:256, 128:] + (last + last.T)))
        both = jnp.where(same_half, both, 0.0)
        other = pltpu.roll(both.reshape(16, 8, 128), 4, 1).reshape(128, 128)
        other = jnp.where(upper, pltpu.roll(other, 4, 1), pltpu.roll(other, 124, 1))
        return both + other

    def finish(pair, carry):
        stages = [pair * 2, pair * 2 + 1]
        with jax.named_scope("fwait"):
            for stage in stages:
                pltpu.make_async_copy(taken.at[stage], taken.at[stage], got.at[stage]).wait()
        with jax.named_scope("comp"):
            wides = [
                jnp.concatenate([taken[stage, :, c].reshape(128, 128) for c in range(8)], axis=1) for stage in stages
            ]
            splits = [parts(wide) for wide in wides]
            grams = [gram_of(split) for split in splits]
            totals = [0.5 * jnp.sum(jnp.where(up == across, gram, 0.0), keepdims=True) for gram in grams]
            scales = [lax.rsqrt(total + 1e-06) for total in totals]
            mixes = mixing([gram * (scale * scale) for gram, scale in zip(grams, scales)], eye, 2)
            mixes = [parts(mix * scale) for mix, scale in zip(mixes, scales)]
            splits = [parts(product(mix, split)) for mix, split in zip(mixes, splits)]
            mixes = mixing([gram_of(split) for split in splits], eye, 3)
            wides = [product(parts(mix), split) for mix, split in zip(mixes, splits)]
            for stage, wide in zip(stages, wides):
                for c in range(8):
                    made[stage, :, c] = wide[:, c * 128 : c * 128 + 128].reshape(16, 8, 128)
        with jax.named_scope("bsend"):
            for stage in stages:
                pltpu.make_async_copy(made.at[stage, row, col], landed.at[stage, me], back_got.at[stage]).start()
                for place in places[::-1]:
                    pltpu.make_async_remote_copy(
                        src_ref=made.at[stage, place[0], place[1]],
                        dst_ref=landed.at[stage, me],
                        send_sem=back_sent.at[stage],
                        recv_sem=back_got.at[stage],
                        device_id=place,
                        device_id_type=MESH,
                    ).start()
        return carry

    lax.fori_loop(0, STAGES // 2, finish, 0)

    weights.wait()
    for stage in range(STAGES):
        with jax.named_scope(f"bwait{stage}"):
            pltpu.make_async_copy(landed.at[stage], landed.at[stage], back_got.at[stage]).wait()
        out_ref[:, stage] = out_ref[:, stage] - learn_rate * landed[stage]
    with jax.named_scope("drain"):
        part = landed.at[0, pl.ds(0, 127)]
        for stage in range(STAGES):
            pltpu.make_async_copy(part, part, sent.at[stage]).wait()
            pltpu.make_async_copy(part, part, back_sent.at[stage]).wait()


def write_out(weights, momentum, weights_out, momentum_out, done):
    copies = [
        pltpu.make_async_copy(weights, weights_out, done.at[0]),
        pltpu.make_async_copy(momentum, momentum_out, done.at[1]),
    ]
    for copy in copies:
        copy.start()
    for copy in copies:
        copy.wait()


def to_tiles(array):
    return array.reshape(512, 4, 2, 128).transpose(0, 2, 1, 3).reshape(128, 4, 8, 128)


def from_tiles(array):
    return array.reshape(512, 2, 4, 128).transpose(0, 2, 1, 3).reshape(512, 4, 256)


def on_device(grad_stack, moment_stack, weight_stack):
    tiles = jax.ShapeDtypeStruct((128, 4, 8, 128), jnp.float32)
    in_vmem = pl.BlockSpec(memory_space=pltpu.VMEM)
    anywhere = pl.BlockSpec(memory_space=pl.ANY)
    updated = pl.pallas_call(
        kernel,
        out_shape=(tiles, tiles),
        in_specs=[anywhere] * 3,
        out_specs=[in_vmem] * 2,
        scratch_shapes=[
            pltpu.VMEM((128, 4, 8, 128), jnp.float32),
            pltpu.VMEM((128, 4, 8, 128), jnp.float32),
            pltpu.VMEM((STAGES, 16, 8, 8, 128), jnp.float32),
            pltpu.VMEM((STAGES, 16, 8, 8, 128), jnp.float32),
            pltpu.VMEM((STAGES, 128, 8, 128), jnp.float32),
            pltpu.SemaphoreType.DMA((STAGES,)),
            pltpu.SemaphoreType.DMA((STAGES,)),
            pltpu.SemaphoreType.DMA((STAGES,)),
            pltpu.SemaphoreType.DMA((STAGES,)),
            pltpu.SemaphoreType.DMA((2, 128 // PIECE)),
            pltpu.SemaphoreType.DMA,
        ],
        compiler_params=pltpu.CompilerParams(
            collective_id=1, has_side_effects=True, vmem_limit_bytes=48 * 1024 * 1024
        ),
    )(to_tiles(grad_stack), to_tiles(moment_stack), to_tiles(weight_stack))
    written = pl.pallas_call(
        write_out,
        out_shape=(tiles, tiles),
        in_specs=[in_vmem] * 2,
        out_specs=[anywhere] * 2,
        scratch_shapes=[pltpu.SemaphoreType.DMA((2,))],
        compiler_params=pltpu.CompilerParams(vmem_limit_bytes=16 * 1024 * 1024),
    )(*updated)
    return tuple(from_tiles(array) for array in written)


def solution(mesh):
    placed = (P(None, "rows", "cols"), P(None, "rows", "cols"), P(None, "rows", "cols"))
    return jax.shard_map(
        on_device,
        mesh=mesh,
        in_specs=placed,
        out_specs=(P(None, "rows", "cols"), P(None, "rows", "cols")),
        check_vma=False,
    )
```

```python
import itertools

import jax
import jax.numpy as jnp
from jax import lax
from jax.experimental import pallas as pl
from jax.experimental.pallas import tpu as pltpu
from jax.sharding import PartitionSpec as P

hold_rate = 0.95
learn_rate = 1.0
LINEAR, CUBIC, QUINTIC = 3.4445, -4.775, 2.0315

MESH = pl.DeviceIdType.MESH
STAGES = 4
PIECE = 16


def send_order():
    def put(axes, values):
        offset = [0, 0, 0]
        for axis, value in zip(axes, values):
            offset[axis] = value % 4
        return tuple(offset)

    rounds = [[(2, 2, 2)]]
    for a, b in itertools.product((1, -1), repeat=2):
        rounds.append([put((0, 1, 2), (1, a, b)), put((0, 1, 2), (-1, -a, -b))])
    for d in range(3):
        e, f = [axis for axis in range(3) if axis != d]
        for a, b in itertools.product((1, -1), repeat=2):
            rounds.append([put((d, e, f), (2, a, b)), put((d, e, f), (0, -a, -b))])
        for a in (1, -1):
            rounds.append([put((d, e, f), (a, 2, 2)), put((d, e, f), (-a, 0, 0))])
        rounds.append([put((d, e, f), (0, 2, 2)), put((d, e, f), (2, 0, 0))])
        for a in (1, -1):
            rounds.append([put((d, e, f), (a, 2, 0)), put((d, e, f), (-a, 0, 2))])
    order = [(0, 0, 0, 1)]
    for group in rounds:
        for core in range(2):
            order += [offset + (core,) for offset in group]
    assert len(set(order)) == 127
    return order


ORDER = send_order()


def parts(array):
    high = array.astype(jnp.bfloat16)
    rest = array - high.astype(jnp.float32)
    middle = rest.astype(jnp.bfloat16)
    return high, middle, (rest - middle.astype(jnp.float32)).astype(jnp.bfloat16)


def product(left, right):
    high, middle, low = left
    high_right, middle_right, low_right = right
    side = lambda *arrays: jnp.concatenate(arrays, axis=1)
    above = lambda *arrays: jnp.concatenate(arrays, axis=0)
    dot = lambda x, y: jnp.dot(x, y, preferred_element_type=jnp.float32)
    large = dot(above(side(high, high), side(middle, middle)), above(high_right, middle_right))
    small = dot(side(low, high), above(high_right, low_right))
    return large[:128] + (large[128:] + small)


def mixing(gram, eye, steps):
    mix = None
    for step in range(steps):
        split = parts(gram)
        poly = LINEAR * eye + CUBIC * gram + QUINTIC * product(split, split)
        split_poly = parts(poly)
        mix = poly if mix is None else product(split_poly, parts(mix))
        if step < steps - 1:
            gram = product(split_poly, parts(product(split_poly, split)))
    return mix


def kernel(
    grad_ref, moment_ref, weight_ref, out_ref, x_ref,
    grad, moment, taken, made, landed, sent, got, back_sent, back_got, loaded, held,
):
    row, col = lax.axis_index("rows"), lax.axis_index("cols")
    z, y, x, core = row // 4, row % 4, col // 2, col % 2
    zs = [lax.rem(z + d, 4) for d in range(4)]
    ys = [lax.rem(y + d, 4) for d in range(4)]
    xs = [lax.rem(x + d, 4) for d in range(4)]
    cores = [core, 1 - core]
    rows = {(a, b): zs[a] * 4 + ys[b] for a in range(4) for b in range(4)}
    cols = {(a, b): xs[a] * 2 + cores[b] for a in range(4) for b in range(2)}
    places = [(rows[dz, dy], cols[dx, dc]) for dz, dy, dx, dc in ORDER]
    me = row * 8 + col

    pieces = [pl.ds(piece * PIECE, PIECE) for piece in range(128 // PIECE)]
    loads = []
    for at, piece in enumerate(pieces):
        loads.append((
            pltpu.make_async_copy(grad_ref.at[piece], grad.at[piece], loaded.at[0, at]),
            pltpu.make_async_copy(moment_ref.at[piece], moment.at[piece], loaded.at[1, at]),
        ))
    for pair in loads:
        for load in pair:
            load.start()
    weights = pltpu.make_async_copy(weight_ref, out_ref, held)
    weights.start()

    with jax.named_scope("greet"):
        barrier = pltpu.get_barrier_semaphore()
        far = sorted(range(127), key=lambda at: -sum(min(d, 4 - d) for d in ORDER[at][:3]))
        for place in [places[at] for at in far]:
            pl.semaphore_signal(barrier, inc=1, device_id=place, device_id_type=MESH)
    with jax.named_scope("momentum"):
        for piece, pair in zip(pieces, loads):
            for load in pair:
                load.wait()
            x_ref[piece] = hold_rate * moment[piece] + grad[piece]
    with jax.named_scope("greetwait"):
        pl.semaphore_wait(barrier, len(places))

    for stage in range(STAGES):
        with jax.named_scope(f"fsend{stage}"):
            pltpu.make_async_copy(x_ref.at[me, stage], taken.at[stage, row, col], got.at[stage]).start()
            for place in places[:: 1 - 2 * (stage % 2)]:
                pltpu.make_async_remote_copy(
                    src_ref=x_ref.at[place[0] * 8 + place[1], stage],
                    dst_ref=taken.at[stage, row, col],
                    send_sem=sent.at[stage],
                    recv_sem=got.at[stage],
                    device_id=place,
                    device_id_type=MESH,
                ).start()

    up = lax.broadcasted_iota(jnp.int32, (128, 128), 0)
    across = lax.broadcasted_iota(jnp.int32, (128, 128), 1)
    same_half = (up // 4) % 2 == (across // 4) % 2
    upper = (across // 4) % 2 == 1
    eye = jnp.where(up == across, 1.0, 0.0).astype(jnp.float32)

    def gram_of(split):
        high, middle, low = split
        both = lax.dot_general(
            jnp.concatenate(split, axis=0), jnp.concatenate((high, middle), axis=0),
            (((1,), (1,)), ((), ())), preferred_element_type=jnp.float32,
        )
        last = both[256:, :128] + both[256:, 128:]
        mixed = both[:128, 128:] + both[128:256, :128]
        both = both[:128, :128] + (mixed + (both[128:256, 128:] + (last + last.T)))
        both = jnp.where(same_half, both, 0.0)
        other = pltpu.roll(both.reshape(16, 8, 128), 4, 1).reshape(128, 128)
        other = jnp.where(upper, pltpu.roll(other, 4, 1), pltpu.roll(other, 124, 1))
        return both + other

    def finish(stage, carry):
        with jax.named_scope("fwait"):
            pltpu.make_async_copy(taken.at[stage], taken.at[stage], got.at[stage]).wait()
        with jax.named_scope("comp"):
            wide = jnp.concatenate([taken[stage, :, c].reshape(128, 128) for c in range(8)], axis=1)
            split = parts(wide)
            gram = gram_of(split)
            total = 0.5 * jnp.sum(jnp.where(up == across, gram, 0.0), keepdims=True)
            scale = lax.rsqrt(total + 1e-06)
            mix = mixing(gram * (scale * scale), eye, 2) * scale
            split = parts(product(parts(mix), split))
            mix = mixing(gram_of(split), eye, 3)
            wide = product(parts(mix), split)
            for c in range(8):
                made[stage, :, c] = wide[:, c * 128 : c * 128 + 128].reshape(16, 8, 128)
        with jax.named_scope("bsend"):
            pltpu.make_async_copy(made.at[stage, row, col], landed.at[stage, me], back_got.at[stage]).start()
            for place in places[::-1]:
                pltpu.make_async_remote_copy(
                    src_ref=made.at[stage, place[0], place[1]],
                    dst_ref=landed.at[stage, me],
                    send_sem=back_sent.at[stage],
                    recv_sem=back_got.at[stage],
                    device_id=place,
                    device_id_type=MESH,
                ).start()
        return carry

    lax.fori_loop(0, STAGES, finish, 0)

    weights.wait()
    for stage in range(STAGES):
        with jax.named_scope(f"bwait{stage}"):
            pltpu.make_async_copy(landed.at[stage], landed.at[stage], back_got.at[stage]).wait()
        out_ref[:, stage] = out_ref[:, stage] - learn_rate * landed[stage]
    with jax.named_scope("drain"):
        part = landed.at[0, pl.ds(0, 127)]
        for stage in range(STAGES):
            pltpu.make_async_copy(part, part, sent.at[stage]).wait()
            pltpu.make_async_copy(part, part, back_sent.at[stage]).wait()


def write_out(weights, momentum, weights_out, momentum_out, done):
    copies = [
        pltpu.make_async_copy(weights, weights_out, done.at[0]),
        pltpu.make_async_copy(momentum, momentum_out, done.at[1]),
    ]
    for copy in copies:
        copy.start()
    for copy in copies:
        copy.wait()


def to_tiles(array):
    return array.reshape(512, 4, 2, 128).transpose(0, 2, 1, 3).reshape(128, 4, 8, 128)


def from_tiles(array):
    return array.reshape(512, 2, 4, 128).transpose(0, 2, 1, 3).reshape(512, 4, 256)


def on_device(grad_stack, moment_stack, weight_stack):
    tiles = jax.ShapeDtypeStruct((128, 4, 8, 128), jnp.float32)
    in_vmem = pl.BlockSpec(memory_space=pltpu.VMEM)
    anywhere = pl.BlockSpec(memory_space=pl.ANY)
    updated = pl.pallas_call(
        kernel,
        out_shape=(tiles, tiles),
        in_specs=[anywhere] * 3,
        out_specs=[in_vmem] * 2,
        scratch_shapes=[
            pltpu.VMEM((128, 4, 8, 128), jnp.float32),
            pltpu.VMEM((128, 4, 8, 128), jnp.float32),
            pltpu.VMEM((STAGES, 16, 8, 8, 128), jnp.float32),
            pltpu.VMEM((STAGES, 16, 8, 8, 128), jnp.float32),
            pltpu.VMEM((STAGES, 128, 8, 128), jnp.float32),
            pltpu.SemaphoreType.DMA((STAGES,)),
            pltpu.SemaphoreType.DMA((STAGES,)),
            pltpu.SemaphoreType.DMA((STAGES,)),
            pltpu.SemaphoreType.DMA((STAGES,)),
            pltpu.SemaphoreType.DMA((2, 128 // PIECE)),
            pltpu.SemaphoreType.DMA,
        ],
        compiler_params=pltpu.CompilerParams(
            collective_id=1, has_side_effects=True, vmem_limit_bytes=48 * 1024 * 1024
        ),
    )(to_tiles(grad_stack), to_tiles(moment_stack), to_tiles(weight_stack))
    written = pl.pallas_call(
        write_out,
        out_shape=(tiles, tiles),
        in_specs=[in_vmem] * 2,
        out_specs=[anywhere] * 2,
        scratch_shapes=[pltpu.SemaphoreType.DMA((2,))],
        compiler_params=pltpu.CompilerParams(vmem_limit_bytes=16 * 1024 * 1024),
    )(*updated)
    return tuple(from_tiles(array) for array in written)


def solution(mesh):
    placed = (P(None, "rows", "cols"), P(None, "rows", "cols"), P(None, "rows", "cols"))
    return jax.shard_map(
        on_device,
        mesh=mesh,
        in_specs=placed,
        out_specs=(P(None, "rows", "cols"), P(None, "rows", "cols")),
        check_vma=False,
    )
```
